32 devices in a mesh: gx: 4 (over y, x), gy: 2 (over core), gz: 4 (over z).
Axes of the slice: x: 2, y: 2, z: 4, core: 2. Of those that a mesh axis runs over, the one named last changes fastest.
Arguments:
- positions: float32 [3, 8, 8, 8, 128], P(None, 'gx', 'gy', 'gz'), may hold values from 0 to 1
- type_ids: int32 [8, 8, 8, 128], P('gx', 'gy', 'gz'), may hold values from 0 to 1
- counts: int32 [8, 8, 8], P('gx', 'gy', 'gz'), may hold values from 64 to 128
- type_charge: float32 [2], replicated, may hold values from -1 to 1
- type_sigma: float32 [2], replicated, may hold values from 0.2 to 0.35
- type_epsilon: float32 [2], replicated, may hold values from 0.05 to 0.5
Outputs:
- forces: float32 [3, 8, 8, 8, 128], P(None, 'gx', 'gy', 'gz')
- totals: float32 [2], replicated
The draws below stay inside these ranges and needn't reach their ends.
All inputs are finite; a program needn't handle non-finite values.
Results may differ from the reference program's by a relative error of at most 0.0003.
Values sent between devices are 32-bit elements; how exact they have to be, the bound alone decides.
A program may use at most 64 MiB of HBM per device.

```python
import math
import jax
import jax.numpy as jnp
from jax import lax

ATOMS_CELL = 128
TYPES = 2
NX = 8
NY = 8
NZ = 8


def plant(result, stream_key, smallest, top_value):
    dims = result.shape
    spot = [jax.random.randint(jax.random.fold_in(stream_key, axis), (), 0, dims[axis]) for axis in range(len(dims))]
    result = result.at[tuple(spot)].set(smallest)
    longest = dims.index(max(dims))
    spot[longest] = (spot[longest] + 1) % dims[longest]
    return result.at[tuple(spot)].set(top_value)


def block_scale(own_key, shape, split, low, high):
    factor_of = 1.0
    for axis_at, shards_of in split:
        steps = jax.random.uniform(jax.random.fold_in(jax.random.fold_in(own_key, 6), axis_at), (shards_of,), jnp.float32, low / len(split), high / len(split))
        factor_of = factor_of * jnp.repeat(jnp.exp(steps), shape[axis_at] // shards_of).reshape((-1,) + (1,) * (len(shape) - 1 - axis_at))
    return factor_of


def setup_inputs(seed: int = 0) -> dict:
    key_of = jax.random.split(jax.random.key(seed), 7)
    return {
        "positions": jnp.clip(1.0 * jax.random.uniform(key_of[0], (3, NX, NY, NZ, ATOMS_CELL), jnp.float32) ** block_scale(key_of[0], (3, NX, NY, NZ, ATOMS_CELL), ((1, 4), (2, 2), (3, 4)), -0.2, 0.2), 0.0, 1.0),
        "type_ids": plant(jax.random.randint(key_of[1], (NX, NY, NZ, ATOMS_CELL), 0, TYPES), jax.random.fold_in(key_of[1], 1), 0, TYPES - 1).astype(jnp.int32),
        "counts": plant(jax.random.randint(key_of[2], (NX, NY, NZ), ATOMS_CELL // 2, ATOMS_CELL + 1), jax.random.fold_in(key_of[2], 1), ATOMS_CELL // 2, ATOMS_CELL).astype(jnp.int32),
        "type_charge": jnp.clip(jax.random.uniform(key_of[3], (TYPES,), jnp.float32, -1.0, 1.0), -1.0, 1.0),
        "type_sigma": jnp.clip(jnp.exp(jax.random.uniform(key_of[4], (TYPES,), jnp.float32, math.log(0.2), math.log(0.35))), 0.2, 0.35),
        "type_epsilon": jnp.clip(jnp.exp(jax.random.uniform(key_of[5], (TYPES,), jnp.float32, math.log(0.05), math.log(0.5))), 0.05, 0.5),
    }


soft_core = 0.09
corner_pairs = [(first_corner, second_corner) for first_corner in range(8) for second_corner in range(8) if first_corner & second_corner == 0 and first_corner <= second_corner]

def corner_of(which):
    return (which & 1, which >> 1 & 1, which >> 2 & 1)

def atom_table(positions, type_ids, counts, type_charge, type_sigma, type_epsilon):
    type_count = type_charge.shape[0]
    kinds_shape = (type_count, 1, 1, 1, 1)
    onehot = (type_ids[None] == jnp.arange(type_count, dtype=jnp.int32).reshape(kinds_shape)).astype(jnp.float32)
    charge = lax.optimization_barrier(jnp.sum(onehot * type_charge.reshape(kinds_shape), 0))
    sigma_atom = lax.optimization_barrier(jnp.sum(onehot * type_sigma.reshape(kinds_shape), 0))
    depth_atom = lax.optimization_barrier(jnp.sum(onehot * jnp.sqrt(type_epsilon).reshape(kinds_shape), 0))
    slots = lax.broadcasted_iota(jnp.int32, type_ids.shape, 3)
    occupied = (slots < counts[..., None]).astype(jnp.float32)
    return jnp.stack([positions[0], positions[1], positions[2], charge, sigma_atom, depth_atom, occupied])

def pair_terms(first, second, offset, selfpair):
    displace = second[:3, :, None, :] - first[:3, :, :, None] + offset[:, None, None, None]
    dist_sq = lax.optimization_barrier(jnp.sum(displace * displace, 0))
    width_atoms = first.shape[-1]
    live_mask = first[6][:, :, None] * second[6][:, None, :] * (dist_sq < 1.0).astype(jnp.float32)
    if selfpair:
        ordered = (lax.broadcasted_iota(jnp.int32, (width_atoms, width_atoms), 0) < lax.broadcasted_iota(jnp.int32, (width_atoms, width_atoms), 1)).astype(jnp.float32)
        live_mask = live_mask * ordered[None]
    sigma_pair = 0.5 * (first[4][:, :, None] + second[4][:, None, :])
    depth_pair = first[5][:, :, None] * second[5][:, None, :]
    coulomb = first[3][:, :, None] * second[3][:, None, :]
    soft_sq = dist_sq + soft_core
    inverse = lax.rsqrt(soft_sq)
    ratio_six = (sigma_pair * sigma_pair / soft_sq) ** 3
    ratio_twelve = ratio_six * ratio_six
    value_here = 4.0 * depth_pair * (ratio_twelve - ratio_six) + coulomb * inverse
    slope_here = (4.0 * depth_pair * (6.0 * ratio_six - 12.0 * ratio_twelve) - coulomb * inverse) * inverse
    cut_sq = 1.0 + soft_core
    cut_len = cut_sq ** 0.5
    cut_six = (sigma_pair * sigma_pair / cut_sq) ** 3
    cut_twelve = cut_six * cut_six
    value_cut = 4.0 * depth_pair * (cut_twelve - cut_six) + coulomb / cut_len
    slope_cut = (4.0 * depth_pair * (6.0 * cut_six - 12.0 * cut_twelve) - coulomb / cut_len) / cut_len
    energy = live_mask * (value_here - value_cut - (soft_sq * inverse - cut_len) * slope_cut)
    slope = live_mask * (slope_here - slope_cut) * inverse
    weighted = slope[None] * displace
    return (lax.optimization_barrier(jnp.sum(weighted, 3)), -lax.optimization_barrier(jnp.sum(weighted, 2)), jnp.sum(energy), jnp.sum(slope * dist_sq))

def reference(positions, type_ids, counts, type_charge, type_sigma, type_epsilon):
    features = atom_table(positions, type_ids, counts, type_charge, type_sigma, type_epsilon)
    forces = jnp.zeros((3, NX, NY, NZ, ATOMS_CELL), jnp.float32)
    energy = jnp.float32(0.0)
    virial = jnp.float32(0.0)

    def rows_of(which):
        shift_x, shift_y, shift_z = corner_of(which)
        shifted = jnp.roll(features, (-shift_x, -shift_y, -shift_z), (1, 2, 3))
        return jnp.transpose(shifted, (1, 2, 0, 3, 4)).reshape((NX * NY, 7, NZ, ATOMS_CELL))

    def placed(force_rows, which):
        shift_x, shift_y, shift_z = corner_of(which)
        grid = jnp.transpose(force_rows.reshape((NX, NY, 3, NZ, ATOMS_CELL)), (2, 0, 1, 3, 4))
        return jnp.roll(grid, (shift_x, shift_y, shift_z), (1, 2, 3))
    for first_corner, second_corner in corner_pairs:
        offset = jnp.array([float(a - b) for a, b in zip(corner_of(second_corner), corner_of(first_corner))], jnp.float32)
        selfpair = first_corner == second_corner

        def one_row(member, offset=offset, selfpair=selfpair):
            return pair_terms(member[0], member[1], offset, selfpair)
        force_first, force_second, energies, virials = lax.map(one_row, (rows_of(first_corner), rows_of(second_corner)))
        forces = forces + placed(force_first, first_corner) + placed(force_second, second_corner)
        energy = energy + jnp.sum(energies)
        virial = virial + jnp.sum(virials)
    normaliser = 1.0 / (NX * NY * NZ * ATOMS_CELL)
    return (forces, jnp.stack([energy, virial]) * normaliser)
```

```python
import functools

import jax
import jax.numpy as jnp
from jax import lax
from jax.experimental import pallas as pl
from jax.experimental.pallas import tpu as pltpu
from jax.sharding import PartitionSpec as P

MESH = pl.DeviceIdType.MESH
AXES = ("gx", "gy", "gz")
soft_core = 0.09
cut_sq = 1.0 + soft_core
cut_len = cut_sq**0.5
second_of = {0: (0, 1, 2, 3, 4, 5, 6, 7), 1: (2, 6), 2: (4, 5), 4: (1, 3)}
direct_limit = 64
VMEM_LIMIT = 56 * 1024 * 1024


def corner_of(which):
    return (which & 1, which >> 1 & 1, which >> 2 & 1)


def neighbour(which, step):
    target = {}
    for axis, bit in zip(AXES, corner_of(which)):
        if bit:
            count = lax.axis_size(axis)
            target[axis] = lax.rem(lax.axis_index(axis) + step + count, count)
    return target


def type_tables(types, shape, charges, sigmas, epsilons):
    def full(value):
        return jnp.full(shape, value, jnp.float32)

    charge = [full(charges[kind]) for kind in range(types)]
    sigma = [full(sigmas[kind]) for kind in range(types)]
    root = [jnp.sqrt(full(epsilons[kind])) for kind in range(types)]
    tables = {}
    for a in range(types):
        for b in range(types):
            sigma_pair = 0.5 * (sigma[a] + sigma[b])
            depth_pair = 4.0 * root[a] * root[b]
            coulomb = charge[a] * charge[b]
            square = sigma_pair * sigma_pair
            sig_six = square * square * square
            six = 6.0 * depth_pair * sig_six
            twelve = 12.0 * depth_pair * sig_six * sig_six
            cut_six, cut_twelve, cut_coulomb = six * cut_sq**-3, twelve * cut_sq**-6, coulomb / cut_len
            shift = ((cut_six - cut_twelve) - cut_coulomb) / cut_len
            level = cut_len * shift - (cut_twelve / 12.0 - cut_six / 6.0 + cut_coulomb)
            tables[a, b] = (twelve, six, coulomb, shift, level)
    return tables


def step_kernel(
    normaliser, types, charges, sigmas, epsilons, positions, type_ids, counts, forces, totals,
    place_in, kind_in, count_in, own, ext, rows, first, table, number_of, force_i, force_j, react, part,
    in_sem, halo_send, halo_recv, back_send, back_recv,
    line, plane, middle, line_send, line_recv, plane_send, plane_recv, *landed,
):
    sizes = own.shape[:3]
    ext_sizes = ext.shape[:3]
    width = own.shape[-1]
    groups = width // 8
    per_cell = 3 + 5 * types
    members = sizes[0] * sizes[1] * sizes[2]
    count_x, count_y, count_z = (lax.axis_size(axis) for axis in AXES)
    at_x, at_y, at_z = (lax.axis_index(axis) for axis in AXES)
    count_plane = count_y * count_z
    at_plane = at_y * count_z + at_z
    direct = count_x * count_plane <= direct_limit
    if direct:
        count_plane, at_plane = count_x * count_plane, at_x * count_plane + at_plane
        count_x, at_x = 1, 0

    def line_target(step):
        return {"gx": lax.rem(at_x + step, count_x)}

    def plane_target(step):
        spot = lax.rem(at_plane + step, count_plane)
        target = {"gy": lax.rem(spot // count_z, count_y), "gz": lax.rem(spot, count_z)}
        if direct:
            target["gx"] = spot // (count_y * count_z)
        return target

    barrier = pltpu.get_barrier_semaphore()
    greeted = count_x - 1 + count_plane - 1
    if not direct:
        greeted += 14
        for which in range(1, 8):
            for step in (1, -1):
                pl.semaphore_signal(barrier, inc=1, device_id=neighbour(which, step), device_id_type=MESH)
    for step in range(1, count_x):
        pl.semaphore_signal(barrier, inc=1, device_id=line_target(step), device_id_type=MESH)
    for step in range(1, count_plane):
        pl.semaphore_signal(barrier, inc=1, device_id=plane_target(step), device_id_type=MESH)

    loads = [
        pltpu.make_async_copy(source, target, in_sem.at[at])
        for at, (source, target) in enumerate(
            ((positions, place_in), (type_ids, kind_in), (counts, count_in))
        )
    ]
    for load in loads:
        load.start()

    cells = [
        (x, y, z)
        for x in range(ext_sizes[0])
        for y in range(ext_sizes[1])
        for z in range(ext_sizes[2])
    ]

    def outside(cell):
        return sum(at == size for at, size in zip(cell, sizes))

    def index_of(x, y, z):
        return (x * ext_sizes[1] + y) * ext_sizes[2] + z

    ordered = sorted(cells, key=outside)
    row_of = {cell: 4 * at for at, cell in enumerate(ordered)}
    inner = [cell for cell in ordered if outside(cell) == 0]
    outer = [cell for cell in ordered if outside(cell) > 0]

    tables = type_tables(types, (8, width), charges, sigmas, epsilons)
    force_j[...] = jnp.zeros(force_j.shape, jnp.float32)
    react[...] = jnp.zeros(react.shape, jnp.float32)
    row_at = lax.broadcasted_iota(jnp.int32, (4, width), 0)
    slot = lax.broadcasted_iota(jnp.int32, (1, width), 1)

    for load in loads:
        load.wait()
    for x, y, z in inner:
        lines = [place_in[axis, x, y, pl.ds(z, 1)] for axis in range(3)]
        kind = kind_in[x, y, pl.ds(z, 1)].astype(jnp.float32)
        held = jnp.broadcast_to(count_in[x, pl.ds(z, 1), pl.ds(y, 1)], (1, width))
        lines.append(jnp.where(slot < held, kind, -1.0))
        tile = jnp.concatenate(lines, 0)
        own[x, y, z] = tile
        ext[x, y, z] = tile

    def build(some):
        for x, y, z in some:
            cell = index_of(x, y, z)
            base = jnp.where(row_at == 0, x, jnp.where(row_at == 1, y, jnp.where(row_at == 2, z, 0)))
            values = ext[x, y, z] + base.astype(jnp.float32)
            for axis in range(3):
                table[cell, axis] = jnp.broadcast_to(values[axis : axis + 1], (8, width))
            parked = (row_at == 0) & (values[3:4] < 0.0)
            rows[pl.ds(row_of[x, y, z], 4)] = jnp.where(parked, x + 4.0, values)
            kind_row = jnp.broadcast_to(values[3:4], (8, width))
            same = [kind_row == float(kind) for kind in range(types)]
            for kind in range(types):
                for at in range(5):
                    picked = jnp.zeros((8, width), jnp.float32)
                    for second_kind in range(types):
                        picked = jnp.where(same[second_kind], tables[kind, second_kind][at], picked)
                    table[cell, 3 + 5 * kind + at] = picked
        leading = [cell for cell in some if outside(cell) <= 1]
        pack = width // 4
        for start in range(0, len(leading), pack):
            batch = leading[start : start + pack]
            turned = jnp.transpose(rows[pl.ds(row_of[batch[0]], width)])
            for at, (x, y, z) in enumerate(batch):
                cell = index_of(x, y, z)
                for axis in range(4):
                    lane = 4 * at + axis
                    spread = jnp.broadcast_to(
                        turned[:, lane : lane + 1], (width, width)
                    ).reshape((groups, 8, width))
                    first[cell, axis] = spread
                for kind in range(1, types):
                    number_of[cell, kind - 1] = jnp.sum((spread == float(kind)).astype(jnp.float32), 0)

    build(inner)

    def interact(own_at, other, kinds, ordered=None):
        xi, yi, zi = own_at
        second = [table[other, at][None] for at in range(per_cell)]

        def chosen(at):
            value = second[3 + at]
            for kind in range(1, types):
                value = jnp.where(kinds[kind - 1], second[3 + 5 * kind + at], value)
            return value

        dx, dy, dz = second[0] - xi, second[1] - yi, second[2] - zi
        soft_sq = jnp.minimum(dx * dx + dy * dy + dz * dz + soft_core, cut_sq)
        inverse = lax.rsqrt(soft_sq)
        inverse_2 = inverse * inverse
        inverse_6 = inverse_2 * inverse_2 * inverse_2
        twelve = chosen(0) * inverse_6 * inverse_6
        six = chosen(1) * inverse_6
        coulomb = chosen(2) * inverse
        shift = chosen(3) * (soft_sq * inverse)
        slope = ((six - twelve) - (coulomb + shift)) * inverse_2
        forces = (slope * dx, slope * dy, slope * dz)
        if ordered is None:
            for axis in range(3):
                force_j[other, axis] -= jnp.sum(forces[axis], 0)
            return forces, (twelve, six, coulomb, shift)
        value = twelve * (1.0 / 12.0) - six * (1.0 / 6.0) + coulomb - shift + chosen(4)
        return forces, jnp.sum(jnp.where(ordered, value, 0.0), 0)

    def role(first_corner, seconds, member, cell_at, energy, depth):
        here = cell_at(first_corner)
        others = [cell_at(which) for which in seconds]
        part_at = tuple(second_of).index(first_corner) + (1 if seconds[0] else 0)
        trips = groups // depth
        slot_at = (
            lax.broadcasted_iota(jnp.int32, (depth, 8, width), 0) * 8
            + lax.broadcasted_iota(jnp.int32, (depth, 8, width), 1)
            - lax.broadcasted_iota(jnp.int32, (depth, 8, width), 2)
        )

        def step(at, energy):
            span = pl.ds(at * depth, depth)
            own_at = tuple(first[here, axis, span] for axis in range(3))
            kind_at = first[here, 3, span]
            kinds = [kind_at == float(kind) for kind in range(1, types)]
            total = None
            sums = None
            for which, other in zip(seconds, others):
                if which == first_corner:
                    forces, own_energy = interact(
                        own_at, other, kinds, slot_at + at * (8 * depth) < 0
                    )
                    energy = energy + own_energy
                else:
                    forces, terms = interact(own_at, other, kinds)
                    terms = [jnp.sum(term, 0) for term in terms]
                    sums = terms if sums is None else [a + b for a, b in zip(sums, terms)]
                total = forces if total is None else [a + b for a, b in zip(total, forces)]
            if sums is not None:
                energy = energy + (
                    (sums[0] * (1.0 / 12.0) - sums[1] * (1.0 / 6.0)) + (sums[2] - sums[3])
                )
            for axis in range(3):
                force_i[part_at, member, axis, span] = total[axis]
            return energy

        energy = lax.fori_loop(0, trips, step, energy)
        for which, other in zip(seconds, others):
            if which != first_corner:
                numbers = [number_of[here, kind - 1] for kind in range(1, types)]
                rest = jnp.full((8, width), float(groups))
                for number in numbers:
                    rest = rest - number
                for kind, number in enumerate([rest, *numbers]):
                    energy = energy + number * table[other, 3 + 5 * kind + 4]
        return energy

    def corners(x0, y0, z0):
        def cell_at(which):
            shift = corner_of(which)
            return index_of(x0 + shift[0], y0 + shift[1], z0 + shift[2])

        return cell_at

    def one_self(member, energy):
        z0 = lax.rem(member, sizes[2])
        y0 = lax.rem(member // sizes[2], sizes[1])
        x0 = member // (sizes[2] * sizes[1])
        return role(0, (0,), member, corners(x0, y0, z0), energy, 4)

    def across(x0, y0, z0, energy):
        member = (x0 * sizes[1] + y0) * sizes[2] + z0
        cell_at = corners(x0, y0, z0)
        for first_corner, seconds in second_of.items():
            seconds = tuple(which for which in seconds if which)
            energy = role(first_corner, seconds, member, cell_at, energy, 2 if first_corner == 0 else 4)
        return energy

    energy = lax.fori_loop(0, members, one_self, jnp.zeros((8, width), jnp.float32))

    pl.semaphore_wait(barrier, greeted)
    halos = []
    for which in range(1, 8):
        bits = corner_of(which)
        source = tuple(pl.ds(0, 1 if bit else size) for bit, size in zip(bits, sizes))
        target = tuple(
            pl.ds(size, 1) if bit else pl.ds(0, size) for bit, size in zip(bits, sizes)
        )
        copy = pltpu.make_async_remote_copy(
            src_ref=own.at[source],
            dst_ref=ext.at[target],
            send_sem=halo_send.at[which],
            recv_sem=halo_recv.at[which],
            device_id=neighbour(which, -1),
            device_id_type=MESH,
        )
        copy.start()
        halos.append(copy)

    less = tuple(size - 1 for size in sizes)

    def inside(at, energy):
        z0 = lax.rem(at, less[2])
        y0 = lax.rem(at // less[2], less[1])
        x0 = at // (less[2] * less[1])
        return across(x0, y0, z0, energy)

    if less[0] * less[1] * less[2]:
        energy = lax.fori_loop(0, less[0] * less[1] * less[2], inside, energy)

    for copy in halos:
        copy.wait()
    build(outer)

    sheet, bar = sizes[1] * sizes[2], less[0] * sizes[2]

    def border(at, energy):
        at_sheet, at_bar, at_rest = at, at - sheet, at - sheet - bar
        on_sheet, on_bar = at < sheet, at < sheet + bar
        x0 = jnp.where(on_sheet, less[0], jnp.where(on_bar, at_bar // sizes[2], at_rest // max(less[1], 1)))
        y0 = jnp.where(on_sheet, at_sheet // sizes[2], jnp.where(on_bar, less[1], lax.rem(at_rest, max(less[1], 1))))
        z0 = jnp.where(on_sheet | on_bar, lax.rem(jnp.where(on_sheet, at_sheet, at_bar), sizes[2]), less[2])
        return across(x0, y0, z0, energy)

    energy = lax.fori_loop(0, sheet + bar + less[0] * less[1], border, energy)

    virial = jnp.zeros((3, width), jnp.float32)

    def reduced(cell):
        x, y, z = cell
        at_cell = index_of(x, y, z)
        held = rows[pl.ds(row_of[cell] + 3, 1)] >= 0.0
        lines = []
        for axis in range(3):
            line = force_j[at_cell, axis]
            partial = None
            for part_at, first_corner in enumerate((0, 0, 1, 2, 4)):
                spot = [at - bit for at, bit in zip(cell, corner_of(first_corner))]
                if all(0 <= at < size for at, size in zip(spot, sizes)):
                    member = (spot[0] * sizes[1] + spot[1]) * sizes[2] + spot[2]
                    value = force_i[part_at, member, axis].reshape((width, width))
                    partial = value if partial is None else partial + value
            if partial is not None:
                turned = jnp.transpose(partial)
                line = line + jnp.sum(turned.reshape((groups, 8, width)), 0)
            line = jnp.sum(line, 0, keepdims=True)
            lines.append(jnp.where(held, line, 0.0))
        return jnp.concatenate(lines, 0)

    for cell in outer:
        force = reduced(cell)
        react[cell[0], cell[1], cell[2], 0:3] = force
        virial = virial - force * rows[pl.ds(row_of[cell], 3)]
    backs = []
    for which in range(1, 8):
        source = tuple(
            pl.ds(size, 1) if bit else pl.ds(0, size)
            for bit, size in zip(corner_of(which), sizes)
        )
        copy = pltpu.make_async_remote_copy(
            src_ref=react.at[source],
            dst_ref=landed[which - 1],
            send_sem=back_send.at[which],
            recv_sem=back_recv.at[which],
            device_id=neighbour(which, 1),
            device_id_type=MESH,
        )
        copy.start()
        backs.append(copy)
    for cell in inner:
        force = reduced(cell)
        react[cell[0], cell[1], cell[2], 0:3] = force
        virial = virial - force * rows[pl.ds(row_of[cell], 3)]
    part[0:1] = jnp.sum(energy, 0, keepdims=True)
    part[1:2] = jnp.sum(virial, 0, keepdims=True)

    def send_plane():
        plane_copies = []
        for step in range(1, count_plane):
            copy = pltpu.make_async_remote_copy(
                src_ref=part if direct else middle,
                dst_ref=plane.at[at_plane],
                send_sem=plane_send.at[step],
                recv_sem=plane_recv.at[step],
                device_id=plane_target(step),
                device_id_type=MESH,
            )
            copy.start()
            plane_copies.append(copy)
        return plane_copies

    if direct:
        plane_copies = send_plane()
        plane[at_plane] = part[...]
    else:
        line_copies = []
        for step in range(1, count_x):
            copy = pltpu.make_async_remote_copy(
                src_ref=part,
                dst_ref=line.at[at_x],
                send_sem=line_send.at[step],
                recv_sem=line_recv.at[step],
                device_id=line_target(step),
                device_id_type=MESH,
            )
            copy.start()
            line_copies.append(copy)
        line[at_x] = part[...]
        for copy in line_copies:
            copy.wait()
        summed = line[0]
        for step in range(1, count_x):
            summed = summed + line[step]
        middle[...] = summed
        plane[at_plane] = summed
        plane_copies = send_plane()
    for copy in backs:
        copy.wait()
    for x, y, z in inner:
        value = react[x, y, z]
        for which in range(1, 8):
            bits = corner_of(which)
            spot = (x, y, z)
            if all(not bit or at == 0 for bit, at in zip(bits, spot)):
                value = value + landed[which - 1][
                    tuple(0 if bit else at for bit, at in zip(bits, spot))
                ]
        for axis in range(3):
            forces[axis, x, y, pl.ds(z, 1)] = value[axis : axis + 1]
    for copy in plane_copies:
        copy.wait()
    summed = plane[0]
    for step in range(1, count_plane):
        summed = summed + plane[step]
    totals[0] = jnp.sum(summed[0:1]) * normaliser
    totals[1] = jnp.sum(summed[1:2]) * normaliser


def per_device(positions, type_ids, counts, type_charge, type_sigma, type_epsilon):
    types = type_charge.shape[0]
    sizes, width = type_ids.shape[:3], type_ids.shape[3]
    ext_sizes = tuple(size + 1 for size in sizes)
    cells = ext_sizes[0] * ext_sizes[1] * ext_sizes[2]
    members = sizes[0] * sizes[1] * sizes[2]
    vmem = pl.BlockSpec(memory_space=pltpu.VMEM)
    smem = pl.BlockSpec(memory_space=pltpu.SMEM)
    hbm = pl.BlockSpec(memory_space=pltpu.HBM)
    f32 = jnp.float32
    count_x, count_y, count_z = (lax.axis_size(axis) for axis in AXES)
    count_plane = count_y * count_z
    slots_x, slots_plane = count_x, count_plane
    if count_x * count_plane <= direct_limit:
        slots_x, slots_plane = 1, count_x * count_plane
    normaliser = 1.0 / (
        sizes[0] * count_x * sizes[1] * count_y * sizes[2] * count_z * width
    )
    landing = [
        pltpu.VMEM(
            tuple(1 if bit else size for bit, size in zip(corner_of(which), sizes)) + (4, width),
            f32,
        )
        for which in range(1, 8)
    ]
    counts = jnp.transpose(counts, (0, 2, 1))
    dma = pltpu.SemaphoreType.DMA
    return pl.pallas_call(
        functools.partial(step_kernel, normaliser, types),
        name="step",
        out_shape=(
            jax.ShapeDtypeStruct((3,) + sizes + (width,), f32),
            jax.ShapeDtypeStruct((2,), f32),
        ),
        in_specs=[smem, smem, smem, hbm, hbm, hbm],
        out_specs=(vmem, smem),
        scratch_shapes=[
            pltpu.VMEM(positions.shape, f32),
            pltpu.VMEM(type_ids.shape, jnp.int32),
            pltpu.VMEM(counts.shape, jnp.int32),
            pltpu.VMEM(sizes + (4, width), f32),
            pltpu.VMEM(ext_sizes + (4, width), f32),
            pltpu.VMEM((4 * cells + width, width), f32),
            pltpu.VMEM((cells, 4, width // 8, 8, width), f32),
            pltpu.VMEM((cells, 3 + 5 * types, 8, width), f32),
            pltpu.VMEM((cells, types - 1, 8, width), f32),
            pltpu.VMEM((1 + len(second_of), members, 3, width // 8, 8, width), f32),
            pltpu.VMEM((cells, 3, 8, width), f32),
            pltpu.VMEM(ext_sizes + (4, width), f32),
            pltpu.VMEM((2, width), f32),
            dma((3,)),
            dma((8,)),
            dma((8,)),
            dma((8,)),
            dma((8,)),
            pltpu.VMEM((slots_x, 2, width), f32),
            pltpu.VMEM((slots_plane, 2, width), f32),
            pltpu.VMEM((2, width), f32),
            dma((slots_x,)),
            dma((slots_x,)),
            dma((slots_plane,)),
            dma((slots_plane,)),
        ]
        + landing,
        compiler_params=pltpu.CompilerParams(
            collective_id=0, has_side_effects=True, vmem_limit_bytes=VMEM_LIMIT
        ),
    )(type_charge, type_sigma, type_epsilon, positions, type_ids, counts)


def solution(mesh):
    in_specs = (
        P(None, "gx", "gy", "gz", None),
        P("gx", "gy", "gz", None),
        P("gx", "gy", "gz"),
        P(),
        P(),
        P(),
    )
    out_specs = (P(None, "gx", "gy", "gz", None), P())
    return jax.shard_map(
        per_device, mesh=mesh, in_specs=in_specs, out_specs=out_specs, check_vma=False
    )
```

```python
import functools

import jax
import jax.numpy as jnp
from jax import lax
from jax.experimental import pallas as pl
from jax.experimental.pallas import tpu as pltpu
from jax.sharding import PartitionSpec as P

MESH = pl.DeviceIdType.MESH
AXES = ("gx", "gy", "gz")
soft_core = 0.09
cut_sq = 1.0 + soft_core
cut_len = cut_sq**0.5
second_of = {0: (0, 1, 2, 3, 4, 5, 6, 7), 1: (2, 6), 2: (4, 5), 4: (1, 3)}
direct_limit = 64
VMEM_LIMIT = 56 * 1024 * 1024


def corner_of(which):
    return (which & 1, which >> 1 & 1, which >> 2 & 1)


def neighbour(which, step):
    target = {}
    for axis, bit in zip(AXES, corner_of(which)):
        if bit:
            count = lax.axis_size(axis)
            target[axis] = lax.rem(lax.axis_index(axis) + step + count, count)
    return target


def type_tables(types, shape, charges, sigmas, epsilons):
    def full(value):
        return jnp.full(shape, value, jnp.float32)

    charge = [full(charges[kind]) for kind in range(types)]
    sigma = [full(sigmas[kind]) for kind in range(types)]
    root = [jnp.sqrt(full(epsilons[kind])) for kind in range(types)]
    tables = {}
    for a in range(types):
        for b in range(types):
            sigma_pair = 0.5 * (sigma[a] + sigma[b])
            depth_pair = 4.0 * root[a] * root[b]
            coulomb = charge[a] * charge[b]
            square = sigma_pair * sigma_pair
            sig_six = square * square * square
            six = 6.0 * depth_pair * sig_six
            twelve = 12.0 * depth_pair * sig_six * sig_six
            cut_six, cut_twelve, cut_coulomb = six * cut_sq**-3, twelve * cut_sq**-6, coulomb / cut_len
            shift = ((cut_six - cut_twelve) - cut_coulomb) / cut_len
            level = cut_len * shift - (cut_twelve / 12.0 - cut_six / 6.0 + cut_coulomb)
            tables[a, b] = (twelve, six, coulomb, shift, level)
    return tables


def step_kernel(
    normaliser, types, charges, sigmas, epsilons, positions, type_ids, counts, forces, totals,
    place_in, kind_in, count_in, own, ext, rows, turn, first, table, number_of, force_i, force_j, react, part,
    in_sem, halo_send, halo_recv, back_send, back_recv,
    line, plane, middle, line_send, line_recv, plane_send, plane_recv, *landed,
):
    sizes = own.shape[:3]
    ext_sizes = ext.shape[:3]
    width = own.shape[-1]
    groups = width // 8
    per_cell = 3 + 5 * types
    members = sizes[0] * sizes[1] * sizes[2]
    count_x, count_y, count_z = (lax.axis_size(axis) for axis in AXES)
    at_x, at_y, at_z = (lax.axis_index(axis) for axis in AXES)
    count_plane = count_y * count_z
    at_plane = at_y * count_z + at_z
    direct = count_x * count_plane <= direct_limit
    loads = [
        pltpu.make_async_copy(source, target, in_sem.at[at])
        for at, (source, target) in enumerate(
            ((positions, place_in), (type_ids, kind_in), (counts, count_in))
        )
    ]
    for load in loads:
        load.start()

    def around(at, count):
        return [at] + [at + step - count * (at + step >= count).astype(jnp.int32) for step in range(1, count)]

    spots = [around(at, count) for at, count in ((at_x, count_x), (at_y, count_y), (at_z, count_z))]
    if direct:
        count_plane, at_plane = count_x * count_plane, at_x * count_plane + at_plane
        count_x, at_x = 1, 0

    def line_target(step):
        return {"gx": spots[0][step]}

    def plane_target(step):
        target = {"gy": spots[1][step // count_z % count_y], "gz": spots[2][step % count_z]}
        if direct:
            target["gx"] = spots[0][step // (count_y * count_z)]
        return target

    barrier = pltpu.get_barrier_semaphore()
    greeted = count_x - 1 + count_plane - 1
    if not direct:
        greeted += 14
        for which in range(1, 8):
            for step in (1, -1):
                pl.semaphore_signal(barrier, inc=1, device_id=neighbour(which, step), device_id_type=MESH)
    for step in range(1, count_x):
        pl.semaphore_signal(barrier, inc=1, device_id=line_target(step), device_id_type=MESH)
    for step in range(1, count_plane):
        pl.semaphore_signal(barrier, inc=1, device_id=plane_target(step), device_id_type=MESH)

    cells = [
        (x, y, z)
        for x in range(ext_sizes[0])
        for y in range(ext_sizes[1])
        for z in range(ext_sizes[2])
    ]

    def outside(cell):
        return sum(at == size for at, size in zip(cell, sizes))

    def index_of(x, y, z):
        return (x * ext_sizes[1] + y) * ext_sizes[2] + z

    ordered = sorted(cells, key=outside)
    row_of = {cell: 4 * at for at, cell in enumerate(ordered)}
    inner = [cell for cell in ordered if outside(cell) == 0]
    outer = [cell for cell in ordered if outside(cell) > 0]

    tables = type_tables(types, (8, width), charges, sigmas, epsilons)
    force_j[...] = jnp.zeros(force_j.shape, jnp.float32)
    react[...] = jnp.zeros(react.shape, jnp.float32)
    row_at = lax.broadcasted_iota(jnp.int32, (4, width), 0)
    slot = lax.broadcasted_iota(jnp.int32, (1, width), 1)

    for load in loads:
        load.wait()
    for x, y, z in inner:
        lines = [place_in[axis, x, y, pl.ds(z, 1)] for axis in range(3)]
        kind = kind_in[x, y, pl.ds(z, 1)].astype(jnp.float32)
        held = jnp.broadcast_to(count_in[x, pl.ds(z, 1), pl.ds(y, 1)], (1, width))
        lines.append(jnp.where(slot < held, kind, -1.0))
        tile = jnp.concatenate(lines, 0)
        own[x, y, z] = tile
        ext[x, y, z] = tile

    def build(some):
        for x, y, z in some:
            cell = index_of(x, y, z)
            base = jnp.where(row_at == 0, x, jnp.where(row_at == 1, y, jnp.where(row_at == 2, z, 0)))
            values = ext[x, y, z] + base.astype(jnp.float32)
            for axis in range(3):
                table[cell, axis] = jnp.broadcast_to(values[axis : axis + 1], (8, width))
            parked = (row_at == 0) & (values[3:4] < 0.0)
            rows[pl.ds(row_of[x, y, z], 4)] = jnp.where(parked, x + 4.0, values)
            kind_row = jnp.broadcast_to(values[3:4], (8, width))
            same = [kind_row == float(kind) for kind in range(types)]
            for kind in range(1, types):
                total = jnp.sum(same[kind].astype(jnp.float32), 1, keepdims=True) * 0.125
                number_of[cell, kind - 1] = jnp.broadcast_to(total, (8, width))
            for kind in range(types):
                for at in range(5):
                    picked = jnp.zeros((8, width), jnp.float32)
                    for second_kind in range(types):
                        picked = jnp.where(same[second_kind], tables[kind, second_kind][at], picked)
                    table[cell, 3 + 5 * kind + at] = picked
        leading = [cell for cell in some if outside(cell) <= 1]
        for at, cell in enumerate(leading):
            lines = rows[pl.ds(row_of[cell], 4)]
            turn[at] = jnp.transpose(jnp.concatenate([lines, lines], 0))
        for axis in range(4):
            for at, (x, y, z) in enumerate(leading):
                first[index_of(x, y, z), axis] = jnp.broadcast_to(
                    turn[at, :, axis : axis + 1], (width, width)
                ).reshape((groups, 8, width))

    build(inner)

    def interact(own_at, other, kinds, ordered=None):
        xi, yi, zi = own_at
        second = [table[other, at][None] for at in range(per_cell)]

        def chosen(at):
            value = second[3 + at]
            for kind in range(1, types):
                value = jnp.where(kinds[kind - 1], second[3 + 5 * kind + at], value)
            return value

        dx, dy, dz = second[0] - xi, second[1] - yi, second[2] - zi
        soft_sq = jnp.minimum(dx * dx + dy * dy + dz * dz + soft_core, cut_sq)
        inverse = lax.rsqrt(soft_sq)
        inverse_2 = inverse * inverse
        inverse_6 = inverse_2 * inverse_2 * inverse_2
        twelve = chosen(0) * inverse_6 * inverse_6
        six = chosen(1) * inverse_6
        coulomb = chosen(2) * inverse
        shift = chosen(3) * (soft_sq * inverse)
        drive = (six - twelve) - (coulomb + shift)
        slope = drive * inverse_2
        forces = (slope * dx, slope * dy, slope * dz)
        for axis in range(3):
            force_j[other, axis] -= jnp.sum(forces[axis], 0)
        if ordered is None:
            terms = (twelve, six, coulomb, shift, slope)
            return forces, [jnp.sum(term, 0) for term in terms]
        value = twelve * (1.0 / 12.0) - six * (1.0 / 6.0) + coulomb - shift + chosen(4)
        pull = drive - soft_core * slope
        return [jnp.sum(jnp.where(ordered, term, 0.0), 0) for term in (value, pull)]

    def slots(depth):
        shape = (depth, 8, width)
        return (
            lax.broadcasted_iota(jnp.int32, shape, 0) * 8
            + lax.broadcasted_iota(jnp.int32, shape, 1)
            - lax.broadcasted_iota(jnp.int32, shape, 2)
        )

    def load_first(here, span):
        own_at = tuple(first[here, axis, span] for axis in range(3))
        kind_at = first[here, 3, span]
        return own_at, [kind_at == float(kind) for kind in range(1, types)]

    def alone(here, sums, depth):
        slot_at = slots(depth)

        def step(at, sums):
            own_at, kinds = load_first(here, pl.ds(at * depth, depth))
            values = interact(own_at, here, kinds, slot_at + at * (8 * depth) < 0)
            return tuple(a + b for a, b in zip(sums, values))

        return lax.fori_loop(0, groups // depth, step, sums)

    def role(first_corner, seconds, member, cell_at, sums, depth):
        here = cell_at(first_corner)
        others = [cell_at(which) for which in seconds]
        part_at = tuple(second_of).index(first_corner)

        def step(at, sums):
            span = pl.ds(at * depth, depth)
            own_at, kinds = load_first(here, span)
            total = None
            parts = None
            for other in others:
                forces, terms = interact(own_at, other, kinds)
                parts = terms if parts is None else [a + b for a, b in zip(parts, terms)]
                total = forces if total is None else [a + b for a, b in zip(total, forces)]
            twelve, six, coulomb, shift, slope = parts
            value = (twelve * (1.0 / 12.0) - six * (1.0 / 6.0)) + (coulomb - shift)
            pull = ((six - twelve) - (coulomb + shift)) - soft_core * slope
            for axis in range(3):
                force_i[part_at, member, axis, span] = total[axis]
            return sums[0] + value, sums[1] + pull

        energy, virial = lax.fori_loop(0, groups // depth, step, sums)
        numbers = [number_of[here, kind - 1] for kind in range(1, types)]
        rest = jnp.full((8, width), float(groups))
        for number in numbers:
            rest = rest - number
        for other in others:
            for kind, number in enumerate([rest, *numbers]):
                energy = energy + number * table[other, 3 + 5 * kind + 4]
        return energy, virial

    def corners(x0, y0, z0):
        def cell_at(which):
            shift = corner_of(which)
            return index_of(x0 + shift[0], y0 + shift[1], z0 + shift[2])

        return cell_at

    def one_self(member, sums):
        z0 = lax.rem(member, sizes[2])
        y0 = lax.rem(member // sizes[2], sizes[1])
        x0 = member // (sizes[2] * sizes[1])
        return alone(index_of(x0, y0, z0), sums, 4)

    def across(x0, y0, z0, sums):
        member = (x0 * sizes[1] + y0) * sizes[2] + z0
        cell_at = corners(x0, y0, z0)
        for first_corner, seconds in second_of.items():
            seconds = tuple(which for which in seconds if which)
            sums = role(first_corner, seconds, member, cell_at, sums, 2 if first_corner == 0 else 4)
        return sums

    blank = jnp.zeros((8, width), jnp.float32)
    sums = lax.fori_loop(0, members, one_self, (blank, blank))

    pl.semaphore_wait(barrier, greeted)
    halos = []
    for which in range(1, 8):
        bits = corner_of(which)
        source = tuple(pl.ds(0, 1 if bit else size) for bit, size in zip(bits, sizes))
        target = tuple(
            pl.ds(size, 1) if bit else pl.ds(0, size) for bit, size in zip(bits, sizes)
        )
        copy = pltpu.make_async_remote_copy(
            src_ref=own.at[source],
            dst_ref=ext.at[target],
            send_sem=halo_send.at[which],
            recv_sem=halo_recv.at[which],
            device_id=neighbour(which, -1),
            device_id_type=MESH,
        )
        copy.start()
        halos.append(copy)

    less = tuple(size - 1 for size in sizes)

    def inside(at, sums):
        z0 = lax.rem(at, less[2])
        y0 = lax.rem(at // less[2], less[1])
        x0 = at // (less[2] * less[1])
        return across(x0, y0, z0, sums)

    if less[0] * less[1] * less[2]:
        sums = lax.fori_loop(0, less[0] * less[1] * less[2], inside, sums)

    for copy in halos:
        copy.wait()
    build(outer)

    def sheet(at, sums):
        return across(less[0], at // sizes[2], lax.rem(at, sizes[2]), sums)

    def border(at, sums):
        on_bar = at < bar
        rest = at - bar
        x0 = jnp.where(on_bar, at // sizes[2], rest // max(less[1], 1))
        y0 = jnp.where(on_bar, less[1], lax.rem(rest, max(less[1], 1)))
        z0 = jnp.where(on_bar, lax.rem(at, sizes[2]), less[2])
        return across(x0, y0, z0, sums)

    def reduced(cell):
        x, y, z = cell
        at_cell = index_of(x, y, z)
        held = rows[pl.ds(row_of[cell] + 3, 1)] >= 0.0
        lines = []
        for axis in range(3):
            line = force_j[at_cell, axis]
            partial = None
            for part_at, first_corner in enumerate(second_of):
                spot = [at - bit for at, bit in zip(cell, corner_of(first_corner))]
                if all(0 <= at < size for at, size in zip(spot, sizes)):
                    member = (spot[0] * sizes[1] + spot[1]) * sizes[2] + spot[2]
                    value = force_i[part_at, member, axis].reshape((width, width))
                    partial = value if partial is None else partial + value
            if partial is not None:
                turned = jnp.transpose(partial)
                line = line + jnp.sum(turned.reshape((groups, 8, width)), 0)
            line = jnp.sum(line, 0, keepdims=True)
            lines.append(jnp.where(held, line, 0.0))
        return jnp.concatenate(lines, 0)

    backs = []

    def give_back(some):
        for cell in outer:
            which = sum((at == size) << bit for bit, (at, size) in enumerate(zip(cell, sizes)))
            if which in some:
                react[cell[0], cell[1], cell[2], 0:3] = reduced(cell)
        for which in some:
            source = tuple(
                pl.ds(size, 1) if bit else pl.ds(0, size)
                for bit, size in zip(corner_of(which), sizes)
            )
            copy = pltpu.make_async_remote_copy(
                src_ref=react.at[source],
                dst_ref=landed[which - 1],
                send_sem=back_send.at[which],
                recv_sem=back_recv.at[which],
                device_id=neighbour(which, 1),
                device_id_type=MESH,
            )
            copy.start()
            backs.append(copy)

    sums = lax.fori_loop(0, sizes[1] * sizes[2], sheet, sums)
    give_back((1, 3, 5, 7))
    bar = less[0] * sizes[2]
    sums = lax.fori_loop(0, bar + less[0] * less[1], border, sums)
    part[0:1] = jnp.sum(sums[0], 0, keepdims=True)
    part[1:2] = jnp.sum(sums[1], 0, keepdims=True)

    def send_plane():
        plane_copies = []
        for step in range(1, count_plane):
            copy = pltpu.make_async_remote_copy(
                src_ref=part if direct else middle,
                dst_ref=plane.at[at_plane],
                send_sem=plane_send.at[step],
                recv_sem=plane_recv.at[step],
                device_id=plane_target(step),
                device_id_type=MESH,
            )
            copy.start()
            plane_copies.append(copy)
        return plane_copies

    if direct:
        plane_copies = send_plane()
        plane[at_plane] = part[...]
    else:
        line_copies = []
        for step in range(1, count_x):
            copy = pltpu.make_async_remote_copy(
                src_ref=part,
                dst_ref=line.at[at_x],
                send_sem=line_send.at[step],
                recv_sem=line_recv.at[step],
                device_id=line_target(step),
                device_id_type=MESH,
            )
            copy.start()
            line_copies.append(copy)
        line[at_x] = part[...]
        for copy in line_copies:
            copy.wait()
        summed = line[0]
        for step in range(1, count_x):
            summed = summed + line[step]
        middle[...] = summed
        plane[at_plane] = summed
        plane_copies = send_plane()
    give_back((2, 4, 6))
    for cell in inner:
        react[cell[0], cell[1], cell[2], 0:3] = reduced(cell)
    for copy in backs:
        copy.wait()
    for x, y, z in inner:
        value = react[x, y, z]
        for which in range(1, 8):
            bits = corner_of(which)
            spot = (x, y, z)
            if all(not bit or at == 0 for bit, at in zip(bits, spot)):
                value = value + landed[which - 1][
                    tuple(0 if bit else at for bit, at in zip(bits, spot))
                ]
        for axis in range(3):
            at = ((axis * sizes[0] + x) * sizes[1] + y) * sizes[2] + z
            forces[pl.ds(at, 1)] = value[axis : axis + 1]
    for copy in plane_copies:
        copy.wait()
    summed = plane[0]
    for step in range(1, count_plane):
        summed = summed + plane[step]
    totals[0] = jnp.sum(summed[0:1]) * normaliser
    totals[1] = jnp.sum(summed[1:2]) * normaliser


def per_device(positions, type_ids, counts, type_charge, type_sigma, type_epsilon):
    types = type_charge.shape[0]
    sizes, width = type_ids.shape[:3], type_ids.shape[3]
    ext_sizes = tuple(size + 1 for size in sizes)
    cells = ext_sizes[0] * ext_sizes[1] * ext_sizes[2]
    members = sizes[0] * sizes[1] * sizes[2]
    vmem = pl.BlockSpec(memory_space=pltpu.VMEM)
    smem = pl.BlockSpec(memory_space=pltpu.SMEM)
    hbm = pl.BlockSpec(memory_space=pltpu.HBM)
    f32 = jnp.float32
    count_x, count_y, count_z = (lax.axis_size(axis) for axis in AXES)
    count_plane = count_y * count_z
    slots_x, slots_plane = count_x, count_plane
    if count_x * count_plane <= direct_limit:
        slots_x, slots_plane = 1, count_x * count_plane
    normaliser = 1.0 / (
        sizes[0] * count_x * sizes[1] * count_y * sizes[2] * count_z * width
    )
    landing = [
        pltpu.VMEM(
            tuple(1 if bit else size for bit, size in zip(corner_of(which), sizes)) + (4, width),
            f32,
        )
        for which in range(1, 8)
    ]
    counts = jnp.transpose(counts, (0, 2, 1))
    dma = pltpu.SemaphoreType.DMA
    forces, totals = pl.pallas_call(
        functools.partial(step_kernel, normaliser, types),
        name="step",
        out_shape=(
            jax.ShapeDtypeStruct((3 * members, width), f32),
            jax.ShapeDtypeStruct((2,), f32),
        ),
        in_specs=[smem, smem, smem, hbm, hbm, hbm],
        out_specs=(vmem, smem),
        scratch_shapes=[
            pltpu.VMEM(positions.shape, f32),
            pltpu.VMEM(type_ids.shape, jnp.int32),
            pltpu.VMEM(counts.shape, jnp.int32),
            pltpu.VMEM(sizes + (4, width), f32),
            pltpu.VMEM(ext_sizes + (4, width), f32),
            pltpu.VMEM((4 * cells, width), f32),
            pltpu.VMEM((cells, width, 8), f32),
            pltpu.VMEM((cells, 4, width // 8, 8, width), f32),
            pltpu.VMEM((cells, 3 + 5 * types, 8, width), f32),
            pltpu.VMEM((cells, types - 1, 8, width), f32),
            pltpu.VMEM((len(second_of), members, 3, width // 8, 8, width), f32),
            pltpu.VMEM((cells, 3, 8, width), f32),
            pltpu.VMEM(ext_sizes + (4, width), f32),
            pltpu.VMEM((2, width), f32),
            dma((3,)),
            dma((8,)),
            dma((8,)),
            dma((8,)),
            dma((8,)),
            pltpu.VMEM((slots_x, 2, width), f32),
            pltpu.VMEM((slots_plane, 2, width), f32),
            pltpu.VMEM((2, width), f32),
            dma((slots_x,)),
            dma((slots_x,)),
            dma((slots_plane,)),
            dma((slots_plane,)),
        ]
        + landing,
        compiler_params=pltpu.CompilerParams(
            collective_id=0, has_side_effects=True, vmem_limit_bytes=VMEM_LIMIT
        ),
    )(type_charge, type_sigma, type_epsilon, positions, type_ids, counts)
    return forces.reshape((3,) + sizes + (width,)), totals


def solution(mesh):
    in_specs = (
        P(None, "gx", "gy", "gz", None),
        P("gx", "gy", "gz", None),
        P("gx", "gy", "gz"),
        P(),
        P(),
        P(),
    )
    out_specs = (P(None, "gx", "gy", "gz", None), P())
    return jax.shard_map(
        per_device, mesh=mesh, in_specs=in_specs, out_specs=out_specs, check_vma=False
    )
```

```python
import functools

import jax
import jax.numpy as jnp
from jax import lax
from jax.experimental import pallas as pl
from jax.experimental.pallas import tpu as pltpu
from jax.sharding import PartitionSpec as P

MESH = pl.DeviceIdType.MESH
AXES = ("gx", "gy", "gz")
soft_core = 0.09
cut_sq = 1.0 + soft_core
cut_len = cut_sq**0.5
second_of = {0: (0, 1, 2, 3, 4, 5, 6, 7), 1: (2, 6), 2: (4, 5), 4: (1, 3)}
direct_limit = 64
far = 1024.0
VMEM_LIMIT = 56 * 1024 * 1024


def corner_of(which):
    return (which & 1, which >> 1 & 1, which >> 2 & 1)


def neighbour(which, step):
    target = {}
    for axis, bit in zip(AXES, corner_of(which)):
        if bit:
            count = lax.axis_size(axis)
            target[axis] = lax.rem(lax.axis_index(axis) + step + count, count)
    return target


def split(value):
    high = value.astype(jnp.bfloat16).astype(jnp.float32)
    rest = value - high
    middle = rest.astype(jnp.bfloat16).astype(jnp.float32)
    return high, middle, rest - middle


def type_tables(types, shape, charges, sigmas, epsilons):
    def full(value):
        return jnp.full(shape, value, jnp.float32)

    charge = [full(charges[kind]) for kind in range(types)]
    sigma = [full(sigmas[kind]) for kind in range(types)]
    root = [jnp.sqrt(full(epsilons[kind])) for kind in range(types)]
    tables = {}
    for a in range(types):
        for b in range(types):
            sigma_pair = 0.5 * (sigma[a] + sigma[b])
            depth_pair = 4.0 * root[a] * root[b]
            coulomb = charge[a] * charge[b]
            square = sigma_pair * sigma_pair
            sig_six = square * square * square
            six = 6.0 * depth_pair * sig_six
            twelve = 12.0 * depth_pair * sig_six * sig_six
            cut_six, cut_twelve, cut_coulomb = six * cut_sq**-3, twelve * cut_sq**-6, coulomb / cut_len
            shift = ((cut_six - cut_twelve) - cut_coulomb) / cut_len
            level = cut_len * shift - (cut_twelve / 12.0 - cut_six / 6.0 + cut_coulomb)
            tables[a, b] = (twelve, six, coulomb, shift, level)
    return tables


def step_kernel(
    normaliser, types, charges, sigmas, epsilons, positions, type_ids, counts, forces, totals,
    place_in, kind_in, count_in, own, ext, rows, turn, left, right, even, odd, first, table, number_of, force_i, force_j, react, part,
    in_sem, halo_send, halo_recv, back_send, back_recv,
    line, plane, middle, line_send, line_recv, plane_send, plane_recv, *landed,
):
    sizes = own.shape[:3]
    ext_sizes = ext.shape[:3]
    width = own.shape[-1]
    groups = width // 8
    per_cell = 3 + 5 * types
    members = sizes[0] * sizes[1] * sizes[2]
    count_x, count_y, count_z = (lax.axis_size(axis) for axis in AXES)
    at_x, at_y, at_z = (lax.axis_index(axis) for axis in AXES)
    count_plane = count_y * count_z
    at_plane = at_y * count_z + at_z
    direct = count_x * count_plane <= direct_limit
    loads = [
        pltpu.make_async_copy(source, target, in_sem.at[at])
        for at, (source, target) in enumerate(
            ((positions, place_in), (type_ids, kind_in), (counts, count_in))
        )
    ]
    for load in loads:
        load.start()

    def around(at, count):
        return [at] + [at + step - count * (at + step >= count).astype(jnp.int32) for step in range(1, count)]

    spots = [around(at, count) for at, count in ((at_x, count_x), (at_y, count_y), (at_z, count_z))]
    if direct:
        count_plane, at_plane = count_x * count_plane, at_x * count_plane + at_plane
        count_x, at_x = 1, 0

    def line_target(step):
        return {"gx": spots[0][step]}

    def plane_target(step):
        target = {"gy": spots[1][step // count_z % count_y], "gz": spots[2][step % count_z]}
        if direct:
            target["gx"] = spots[0][step // (count_y * count_z)]
        return target

    barrier = pltpu.get_barrier_semaphore()
    greeted = count_x - 1 + count_plane - 1
    if not direct:
        greeted += 14
        for which in range(1, 8):
            for step in (1, -1):
                pl.semaphore_signal(barrier, inc=1, device_id=neighbour(which, step), device_id_type=MESH)
    for step in range(1, count_x):
        pl.semaphore_signal(barrier, inc=1, device_id=line_target(step), device_id_type=MESH)
    for step in range(1, count_plane):
        pl.semaphore_signal(barrier, inc=1, device_id=plane_target(step), device_id_type=MESH)

    cells = [
        (x, y, z)
        for x in range(ext_sizes[0])
        for y in range(ext_sizes[1])
        for z in range(ext_sizes[2])
    ]

    def outside(cell):
        return sum(at == size for at, size in zip(cell, sizes))

    def index_of(x, y, z):
        return (x * ext_sizes[1] + y) * ext_sizes[2] + z

    ordered = sorted(cells, key=outside)
    row_of = {cell: 4 * at for at, cell in enumerate(ordered)}
    inner = [cell for cell in ordered if outside(cell) == 0]
    outer = [cell for cell in ordered if outside(cell) > 0]

    tables = type_tables(types, (8, width), charges, sigmas, epsilons)
    force_j[...] = jnp.zeros(force_j.shape, jnp.float32)
    react[...] = jnp.zeros(react.shape, jnp.float32)
    row_at = lax.broadcasted_iota(jnp.int32, (4, width), 0)
    slot = lax.broadcasted_iota(jnp.int32, (1, width), 1)

    for load in loads:
        load.wait()
    for x, y, z in inner:
        lines = [place_in[axis, x, y, pl.ds(z, 1)] for axis in range(3)]
        kind = kind_in[x, y, pl.ds(z, 1)].astype(jnp.float32)
        held = jnp.broadcast_to(count_in[x, pl.ds(z, 1), pl.ds(y, 1)], (1, width))
        lines.append(jnp.where(slot < held, kind, -1.0))
        tile = jnp.concatenate(lines, 0)
        own[x, y, z] = tile
        ext[x, y, z] = tile

    row = lax.broadcasted_iota(jnp.int32, (8, width), 0)
    low, top = row % 4, row < 4

    def build(some):
        for x, y, z in some:
            cell = index_of(x, y, z)
            base = jnp.where(row_at == 0, x, jnp.where(row_at == 1, y, jnp.where(row_at == 2, z, 0)))
            values = ext[x, y, z] + base.astype(jnp.float32)
            for axis in range(3):
                table[cell, axis] = jnp.broadcast_to(values[axis : axis + 1], (8, width))
            parked = (row_at == 0) & (values[3:4] < 0.0)
            lines = jnp.where(parked, x + 4.0, values)
            rows[pl.ds(row_of[x, y, z], 4)] = lines
            middle = [0.5 * size for size in ext_sizes]
            shift = jnp.where(low == 0, middle[0], jnp.where(low == 1, middle[1], middle[2]))
            both = jnp.concatenate([values, values], 0)
            live = jnp.broadcast_to(values[3:4], (8, width)) >= 0.0
            place = jnp.where(live & (low < 3), both - shift, 0.0)
            norm = jnp.sum((place * place)[0:4], 0, keepdims=True)
            norm = jnp.where(live, jnp.broadcast_to(norm, (8, width)), far)
            high, mid, tiny = split(jnp.where(low == 3, norm, place))
            twice, twice_mid, twice_tiny = split(jnp.where(low == 3, norm + soft_core, -2.0 * place))
            high_one = jnp.where(row == 3, 1.0, high)
            twice_one = jnp.where(row == 3, 1.0, twice)
            right[cell] = jnp.concatenate(
                [
                    jnp.where(top, twice_one, jnp.where(row == 7, twice, twice_mid)),
                    jnp.where(top, twice_one, twice_mid),
                    jnp.where(top, twice_tiny, jnp.where(row == 7, 1.0, twice)),
                    jnp.zeros((8, width), jnp.float32),
                ],
                0,
            ).astype(jnp.bfloat16)
            if outside((x, y, z)) <= 1:
                turned = jnp.transpose(
                    jnp.concatenate(
                        [
                            jnp.where(row == 7, 1.0, high),
                            jnp.where(row == 7, 1.0, mid),
                            jnp.where(top, high_one, tiny),
                            jnp.concatenate([lines, lines], 0),
                        ],
                        0,
                    )
                )
                left[cell] = turned.astype(jnp.bfloat16)
                turn[cell] = turned
            kind_row = jnp.broadcast_to(values[3:4], (8, width))
            same = [kind_row == float(kind) for kind in range(types)]
            for kind in range(1, types):
                total = jnp.sum(same[kind].astype(jnp.float32), 1, keepdims=True) * 0.125
                number_of[cell, kind - 1] = jnp.broadcast_to(total, (8, width))
            for kind in range(types):
                for at in range(5):
                    picked = jnp.zeros((8, width), jnp.float32)
                    for second_kind in range(types):
                        picked = jnp.where(same[second_kind], tables[kind, second_kind][at], picked)
                    table[cell, 3 + 5 * kind + at] = picked
        leading = [cell for cell in some if outside(cell) <= 1]
        for axis in range(4):
            for cell in leading:
                at = index_of(*cell)
                first[at, axis] = jnp.broadcast_to(
                    turn[at, :, 24 + axis : 25 + axis], (width, width)
                ).reshape((groups, 8, width))

    build(inner)

    def interact(own_at, other, kinds, soft_sq=None, ordered=None):
        xi, yi, zi = own_at
        second = [table[other, at][None] for at in range(per_cell)]

        def chosen(at):
            value = second[3 + at]
            for kind in range(1, types):
                value = jnp.where(kinds[kind - 1], second[3 + 5 * kind + at], value)
            return value

        dx, dy, dz = second[0] - xi, second[1] - yi, second[2] - zi
        if soft_sq is None:
            soft_sq = dx * dx + dy * dy + dz * dz + soft_core
        soft_sq = jnp.minimum(soft_sq, cut_sq)
        inverse = lax.rsqrt(soft_sq)
        inverse_2 = inverse * inverse
        inverse_6 = inverse_2 * inverse_2 * inverse_2
        twelve = chosen(0) * inverse_6 * inverse_6
        six = chosen(1) * inverse_6
        coulomb = chosen(2) * inverse
        shift = chosen(3) * (soft_sq * inverse)
        drive = (six - twelve) - (coulomb + shift)
        slope = drive * inverse_2
        forces = (slope * dx, slope * dy, slope * dz)
        for axis in range(3):
            force_j[other, axis] -= jnp.sum(forces[axis], 0)
        if ordered is None:
            terms = (twelve, six, coulomb, shift, slope)
            return forces, [jnp.sum(term, 0) for term in terms]
        value = twelve * (1.0 / 12.0) - six * (1.0 / 6.0) + coulomb - shift + chosen(4)
        pull = drive - soft_core * slope
        return [jnp.sum(jnp.where(ordered, term, 0.0), 0) for term in (value, pull)]

    def slots(depth):
        shape = (depth, 8, width)
        return (
            lax.broadcasted_iota(jnp.int32, shape, 0) * 8
            + lax.broadcasted_iota(jnp.int32, shape, 1)
            - lax.broadcasted_iota(jnp.int32, shape, 2)
        )

    def load_first(here, span):
        own_at = tuple(first[here, axis, span] for axis in range(3))
        kind_at = first[here, 3, span]
        return own_at, [kind_at == float(kind) for kind in range(1, types)]

    def alone(here, sums, depth):
        slot_at = slots(depth)

        def step(at, sums):
            own_at, kinds = load_first(here, pl.ds(at * depth, depth))
            values = interact(own_at, here, kinds, ordered=slot_at + at * (8 * depth) < 0)
            return tuple(a + b for a, b in zip(sums, values))

        return lax.fori_loop(0, groups // depth, step, sums)

    def levels(energy, here, others):
        numbers = [number_of[here, kind - 1] for kind in range(1, types)]
        rest = jnp.full((8, width), float(groups))
        for number in numbers:
            rest = rest - number
        for other in others:
            for kind, number in enumerate([rest, *numbers]):
                energy = energy + number * table[other, 3 + 5 * kind + 4]
        return energy

    roles = {
        first_corner: tuple(which for which in seconds if which)
        for first_corner, seconds in second_of.items()
    }
    depth = 4
    trips = groups // depth
    offset_of = {}
    for first_corner, seconds in roles.items():
        offset_of[first_corner] = sum(len(roles[corner]) for corner in offset_of)

    def distances(store, cell_at, chunk, first_corner):
        wide = 8 * depth
        lefts = left[cell_at(first_corner), pl.ds(chunk * wide, wide)]
        seconds = roles[first_corner]
        for at in range(0, len(seconds), 2):
            some = [right[cell_at(which)] for which in seconds[at : at + 2]]
            found = jnp.dot(
                lefts,
                jnp.concatenate(some, 1) if len(some) > 1 else some[0],
                preferred_element_type=jnp.float32,
            )
            for n in range(len(some)):
                store[offset_of[first_corner] + at + n, pl.ds(chunk * depth, depth)] = found[:, n * width : (n + 1) * width].reshape(
                    (depth, 8, width)
                )

    def role(first_corner, member, cell_at, chunk, held, sums):
        here = cell_at(first_corner)
        part_at = tuple(second_of).index(first_corner)
        fine = 4 if first_corner == 0 else 4
        for start in range(0, depth, fine):
            span = pl.ds(chunk * depth + start, fine)
            own_at, kinds = load_first(here, span)
            total = None
            parts = None
            for n, which in enumerate(roles[first_corner]):
                forces, terms = interact(
                    own_at,
                    cell_at(which),
                    kinds,
                    held[offset_of[first_corner] + n, pl.ds(chunk * depth + start, fine)],
                )
                parts = terms if parts is None else [a + b for a, b in zip(parts, terms)]
                total = forces if total is None else [a + b for a, b in zip(total, forces)]
            twelve, six, coulomb, shift, slope = parts
            value = (twelve * (1.0 / 12.0) - six * (1.0 / 6.0)) + (coulomb - shift)
            pull = ((six - twelve) - (coulomb + shift)) - soft_core * slope
            for axis in range(3):
                force_i[part_at, member, axis, span] = total[axis]
            sums = sums[0] + value, sums[1] + pull
        return sums

    def corners(x0, y0, z0):
        def cell_at(which):
            shift = corner_of(which)
            return index_of(x0 + shift[0], y0 + shift[1], z0 + shift[2])

        return cell_at

    def one_self(member, sums):
        z0 = lax.rem(member, sizes[2])
        y0 = lax.rem(member // sizes[2], sizes[1])
        x0 = member // (sizes[2] * sizes[1])
        return alone(index_of(x0, y0, z0), sums, 4)

    def across(homes, sums):
        stores = (even, odd)
        for first_corner in roles:
            for chunk in range(trips):
                distances(even, corners(*homes[0]), chunk, first_corner)
        for at, (x0, y0, z0) in enumerate(homes):
            member = (x0 * sizes[1] + y0) * sizes[2] + z0
            cell_at = corners(x0, y0, z0)
            held, store = stores[at % 2], stores[(at + 1) % 2]
            after = corners(*homes[at + 1]) if at + 1 < len(homes) else None

            def step(chunk, sums, some):
                for first_corner in some:
                    if after is not None:
                        distances(store, after, chunk, first_corner)
                for first_corner in some:
                    sums = role(first_corner, member, cell_at, chunk, held, sums)
                return sums

            for some in ((0,), tuple(corner for corner in roles if corner)):
                sums = lax.fori_loop(0, trips, functools.partial(step, some=some), sums)
        return sums

    blank = jnp.zeros((8, width), jnp.float32)
    sums = lax.fori_loop(0, members, one_self, (blank, blank))

    def base_level(member, energy):
        z0 = lax.rem(member, sizes[2])
        y0 = lax.rem(member // sizes[2], sizes[1])
        x0 = member // (sizes[2] * sizes[1])
        cell_at = corners(x0, y0, z0)
        for first_corner, seconds in roles.items():
            energy = levels(energy, cell_at(first_corner), [cell_at(which) for which in seconds])
        return energy


    pl.semaphore_wait(barrier, greeted)
    halos = []
    for which in range(1, 8):
        bits = corner_of(which)
        source = tuple(pl.ds(0, 1 if bit else size) for bit, size in zip(bits, sizes))
        target = tuple(
            pl.ds(size, 1) if bit else pl.ds(0, size) for bit, size in zip(bits, sizes)
        )
        copy = pltpu.make_async_remote_copy(
            src_ref=own.at[source],
            dst_ref=ext.at[target],
            send_sem=halo_send.at[which],
            recv_sem=halo_recv.at[which],
            device_id=neighbour(which, -1),
            device_id_type=MESH,
        )
        copy.start()
        halos.append(copy)

    less = tuple(size - 1 for size in sizes)

    homes = [
        (x, y, z) for x in range(sizes[0]) for y in range(sizes[1]) for z in range(sizes[2])
    ]
    inside = [home for home in homes if all(at < most for at, most in zip(home, less))]
    sheet = [home for home in homes if home[0] == less[0]]
    border = [home for home in homes if home not in inside and home not in sheet]
    if inside:
        sums = across(inside, sums)

    for copy in halos:
        copy.wait()
    build(outer)

    def reduced(cell):
        x, y, z = cell
        at_cell = index_of(x, y, z)
        held = rows[pl.ds(row_of[cell] + 3, 1)] >= 0.0
        lines = []
        for axis in range(3):
            line = force_j[at_cell, axis]
            partial = None
            for part_at, first_corner in enumerate(second_of):
                spot = [at - bit for at, bit in zip(cell, corner_of(first_corner))]
                if all(0 <= at < size for at, size in zip(spot, sizes)):
                    member = (spot[0] * sizes[1] + spot[1]) * sizes[2] + spot[2]
                    value = force_i[part_at, member, axis].reshape((width, width))
                    partial = value if partial is None else partial + value
            if partial is not None:
                turned = jnp.transpose(partial)
                line = line + jnp.sum(turned.reshape((groups, 8, width)), 0)
            line = jnp.sum(line, 0, keepdims=True)
            lines.append(jnp.where(held, line, 0.0))
        return jnp.concatenate(lines, 0)

    backs = []

    def give_back(some):
        for cell in outer:
            which = sum((at == size) << bit for bit, (at, size) in enumerate(zip(cell, sizes)))
            if which in some:
                react[cell[0], cell[1], cell[2], 0:3] = reduced(cell)
        for which in some:
            source = tuple(
                pl.ds(size, 1) if bit else pl.ds(0, size)
                for bit, size in zip(corner_of(which), sizes)
            )
            copy = pltpu.make_async_remote_copy(
                src_ref=react.at[source],
                dst_ref=landed[which - 1],
                send_sem=back_send.at[which],
                recv_sem=back_recv.at[which],
                device_id=neighbour(which, 1),
                device_id_type=MESH,
            )
            copy.start()
            backs.append(copy)

    sums = across(sheet, sums)
    give_back((1, 3, 5, 7))
    energy = lax.fori_loop(0, members, base_level, sums[0])
    sums = energy, sums[1]
    if border:
        sums = across(border, sums)
    part[0:1] = jnp.sum(sums[0], 0, keepdims=True)
    part[1:2] = jnp.sum(sums[1], 0, keepdims=True)

    def send_plane():
        plane_copies = []
        for step in range(1, count_plane):
            copy = pltpu.make_async_remote_copy(
                src_ref=part if direct else middle,
                dst_ref=plane.at[at_plane],
                send_sem=plane_send.at[step],
                recv_sem=plane_recv.at[step],
                device_id=plane_target(step),
                device_id_type=MESH,
            )
            copy.start()
            plane_copies.append(copy)
        return plane_copies

    if direct:
        plane_copies = send_plane()
        plane[at_plane] = part[...]
    else:
        line_copies = []
        for step in range(1, count_x):
            copy = pltpu.make_async_remote_copy(
                src_ref=part,
                dst_ref=line.at[at_x],
                send_sem=line_send.at[step],
                recv_sem=line_recv.at[step],
                device_id=line_target(step),
                device_id_type=MESH,
            )
            copy.start()
            line_copies.append(copy)
        line[at_x] = part[...]
        for copy in line_copies:
            copy.wait()
        summed = line[0]
        for step in range(1, count_x):
            summed = summed + line[step]
        middle[...] = summed
        plane[at_plane] = summed
        plane_copies = send_plane()
    give_back((2, 4, 6))
    for cell in inner:
        react[cell[0], cell[1], cell[2], 0:3] = reduced(cell)
    for copy in backs:
        copy.wait()
    for x, y, z in inner:
        value = react[x, y, z]
        for which in range(1, 8):
            bits = corner_of(which)
            spot = (x, y, z)
            if all(not bit or at == 0 for bit, at in zip(bits, spot)):
                value = value + landed[which - 1][
                    tuple(0 if bit else at for bit, at in zip(bits, spot))
                ]
        for axis in range(3):
            at = ((axis * sizes[0] + x) * sizes[1] + y) * sizes[2] + z
            forces[pl.ds(at, 1)] = value[axis : axis + 1]
    for copy in plane_copies:
        copy.wait()
    summed = plane[0]
    for step in range(1, count_plane):
        summed = summed + plane[step]
    totals[0] = jnp.sum(summed[0:1]) * normaliser
    totals[1] = jnp.sum(summed[1:2]) * normaliser


def per_device(positions, type_ids, counts, type_charge, type_sigma, type_epsilon):
    types = type_charge.shape[0]
    sizes, width = type_ids.shape[:3], type_ids.shape[3]
    ext_sizes = tuple(size + 1 for size in sizes)
    cells = ext_sizes[0] * ext_sizes[1] * ext_sizes[2]
    members = sizes[0] * sizes[1] * sizes[2]
    vmem = pl.BlockSpec(memory_space=pltpu.VMEM)
    smem = pl.BlockSpec(memory_space=pltpu.SMEM)
    hbm = pl.BlockSpec(memory_space=pltpu.HBM)
    f32 = jnp.float32
    count_x, count_y, count_z = (lax.axis_size(axis) for axis in AXES)
    count_plane = count_y * count_z
    slots_x, slots_plane = count_x, count_plane
    if count_x * count_plane <= direct_limit:
        slots_x, slots_plane = 1, count_x * count_plane
    normaliser = 1.0 / (
        sizes[0] * count_x * sizes[1] * count_y * sizes[2] * count_z * width
    )
    landing = [
        pltpu.VMEM(
            tuple(1 if bit else size for bit, size in zip(corner_of(which), sizes)) + (4, width),
            f32,
        )
        for which in range(1, 8)
    ]
    counts = jnp.transpose(counts, (0, 2, 1))
    dma = pltpu.SemaphoreType.DMA
    forces, totals = pl.pallas_call(
        functools.partial(step_kernel, normaliser, types),
        name="step",
        out_shape=(
            jax.ShapeDtypeStruct((3 * members, width), f32),
            jax.ShapeDtypeStruct((2,), f32),
        ),
        in_specs=[smem, smem, smem, hbm, hbm, hbm],
        out_specs=(vmem, smem),
        scratch_shapes=[
            pltpu.VMEM(positions.shape, f32),
            pltpu.VMEM(type_ids.shape, jnp.int32),
            pltpu.VMEM(counts.shape, jnp.int32),
            pltpu.VMEM(sizes + (4, width), f32),
            pltpu.VMEM(ext_sizes + (4, width), f32),
            pltpu.VMEM((4 * cells, width), f32),
            pltpu.VMEM((cells, width, 32), f32),
            pltpu.VMEM((cells, width, 32), jnp.bfloat16),
            pltpu.VMEM((cells, 32, width), jnp.bfloat16),
            pltpu.VMEM((13, width // 8, 8, width), f32),
            pltpu.VMEM((13, width // 8, 8, width), f32),
            pltpu.VMEM((cells, 4, width // 8, 8, width), f32),
            pltpu.VMEM((cells, 3 + 5 * types, 8, width), f32),
            pltpu.VMEM((cells, types - 1, 8, width), f32),
            pltpu.VMEM((len(second_of), members, 3, width // 8, 8, width), f32),
            pltpu.VMEM((cells, 3, 8, width), f32),
            pltpu.VMEM(ext_sizes + (4, width), f32),
            pltpu.VMEM((2, width), f32),
            dma((3,)),
            dma((8,)),
            dma((8,)),
            dma((8,)),
            dma((8,)),
            pltpu.VMEM((slots_x, 2, width), f32),
            pltpu.VMEM((slots_plane, 2, width), f32),
            pltpu.VMEM((2, width), f32),
            dma((slots_x,)),
            dma((slots_x,)),
            dma((slots_plane,)),
            dma((slots_plane,)),
        ]
        + landing,
        compiler_params=pltpu.CompilerParams(
            collective_id=0, has_side_effects=True, vmem_limit_bytes=VMEM_LIMIT
        ),
    )(type_charge, type_sigma, type_epsilon, positions, type_ids, counts)
    return forces.reshape((3,) + sizes + (width,)), totals


def solution(mesh):
    in_specs = (
        P(None, "gx", "gy", "gz", None),
        P("gx", "gy", "gz", None),
        P("gx", "gy", "gz"),
        P(),
        P(),
        P(),
    )
    out_specs = (P(None, "gx", "gy", "gz", None), P())
    return jax.shard_map(
        per_device, mesh=mesh, in_specs=in_specs, out_specs=out_specs, check_vma=False
    )
```

```python
import functools

import jax
import jax.numpy as jnp
from jax import lax
from jax.experimental import pallas as pl
from jax.experimental.pallas import tpu as pltpu
from jax.sharding import PartitionSpec as P

MESH = pl.DeviceIdType.MESH
AXES = ("gx", "gy", "gz")
soft_core = 0.09
cut_sq = 1.0 + soft_core
cut_len = cut_sq**0.5
second_of = {0: (0, 1, 2, 3, 4, 5, 6, 7), 1: (2, 6), 2: (4, 5), 4: (1, 3)}
direct_limit = 64
far = 1024.0
VMEM_LIMIT = 40 * 1024 * 1024


def corner_of(which):
    return (which & 1, which >> 1 & 1, which >> 2 & 1)


def neighbour(which, step):
    target = {}
    for axis, bit in zip(AXES, corner_of(which)):
        if bit:
            count = lax.axis_size(axis)
            target[axis] = lax.rem(lax.axis_index(axis) + step + count, count)
    return target


def split(value):
    high = value.astype(jnp.bfloat16).astype(jnp.float32)
    rest = value - high
    middle = rest.astype(jnp.bfloat16).astype(jnp.float32)
    return high, middle, rest - middle


def type_tables(types, shape, charges, sigmas, epsilons):
    def full(value):
        return jnp.full(shape, value, jnp.float32)

    charge = [full(charges[kind]) for kind in range(types)]
    sigma = [full(sigmas[kind]) for kind in range(types)]
    root = [jnp.sqrt(full(epsilons[kind])) for kind in range(types)]
    tables = {}
    for a in range(types):
        for b in range(types):
            sigma_pair = 0.5 * (sigma[a] + sigma[b])
            depth_pair = 4.0 * root[a] * root[b]
            coulomb = charge[a] * charge[b]
            square = sigma_pair * sigma_pair
            sig_six = square * square * square
            six = 6.0 * depth_pair * sig_six
            twelve = 12.0 * depth_pair * sig_six * sig_six
            cut_six, cut_twelve, cut_coulomb = six * cut_sq**-3, twelve * cut_sq**-6, coulomb / cut_len
            shift = ((cut_six - cut_twelve) - cut_coulomb) / cut_len
            level = cut_len * shift - (cut_twelve / 12.0 - cut_six / 6.0 + cut_coulomb)
            tables[a, b] = (twelve, six, coulomb, shift, level)
    return tables


def step_kernel(
    normaliser, types, charges, sigmas, epsilons, positions, type_ids, counts, forces, totals,
    place_in, kind_in, count_in, own, ext, rows, pick, left, right, even, odd, first, table, number_of, force_i, force_j, react, part,
    in_sem, halo_send, halo_recv, back_send, back_recv,
    line, plane, middle, line_send, line_recv, plane_send, plane_recv, *landed,
):
    sizes = own.shape[:3]
    ext_sizes = ext.shape[:3]
    width = own.shape[-1]
    groups = width // 8
    per_cell = 3 + 5 * types
    members = sizes[0] * sizes[1] * sizes[2]
    count_x, count_y, count_z = (lax.axis_size(axis) for axis in AXES)
    at_x, at_y, at_z = (lax.axis_index(axis) for axis in AXES)
    count_plane = count_y * count_z
    at_plane = at_y * count_z + at_z
    direct = count_x * count_plane <= direct_limit
    loads = [
        pltpu.make_async_copy(source, target, in_sem.at[at])
        for at, (source, target) in enumerate(
            ((positions, place_in), (type_ids, kind_in), (counts, count_in))
        )
    ]
    for load in loads:
        load.start()

    def around(at, count):
        return [at] + [at + step - count * (at + step >= count).astype(jnp.int32) for step in range(1, count)]

    spots = [around(at, count) for at, count in ((at_x, count_x), (at_y, count_y), (at_z, count_z))]
    if direct:
        count_plane, at_plane = count_x * count_plane, at_x * count_plane + at_plane
        count_x, at_x = 1, 0

    def line_target(step):
        return {"gx": spots[0][step]}

    def plane_target(step):
        target = {"gy": spots[1][step // count_z % count_y], "gz": spots[2][step % count_z]}
        if direct:
            target["gx"] = spots[0][step // (count_y * count_z)]
        return target

    barrier = pltpu.get_barrier_semaphore()
    greeted = count_x - 1 + count_plane - 1
    if not direct:
        greeted += 14
        for which in range(1, 8):
            for step in (1, -1):
                pl.semaphore_signal(barrier, inc=1, device_id=neighbour(which, step), device_id_type=MESH)
    for step in range(1, count_x):
        pl.semaphore_signal(barrier, inc=1, device_id=line_target(step), device_id_type=MESH)
    for step in range(1, count_plane):
        pl.semaphore_signal(barrier, inc=1, device_id=plane_target(step), device_id_type=MESH)

    cells = [
        (x, y, z)
        for x in range(ext_sizes[0])
        for y in range(ext_sizes[1])
        for z in range(ext_sizes[2])
    ]

    def outside(cell):
        return sum(at == size for at, size in zip(cell, sizes))

    def index_of(x, y, z):
        return (x * ext_sizes[1] + y) * ext_sizes[2] + z

    ordered = sorted(cells, key=outside)
    row_of = {cell: at for at, cell in enumerate(ordered)}
    inner = [cell for cell in ordered if outside(cell) == 0]
    outer = [cell for cell in ordered if outside(cell) > 0]

    tables = type_tables(types, (8, width), charges, sigmas, epsilons)
    force_j[...] = jnp.zeros(force_j.shape, jnp.float32)
    react[...] = jnp.zeros(react.shape, jnp.float32)
    slot = lax.broadcasted_iota(jnp.int32, (1, width), 1)

    for load in loads:
        load.wait()
    for x, y, z in inner:
        lines = [place_in[axis, x, y, pl.ds(z, 1)] for axis in range(3)]
        kind = kind_in[x, y, pl.ds(z, 1)].astype(jnp.float32)
        held = jnp.broadcast_to(count_in[x, pl.ds(z, 1), pl.ds(y, 1)], (1, width))
        lines.append(jnp.where(slot < held, kind, -1.0))
        tile = jnp.concatenate(lines, 0)
        own[x, y, z] = tile
        ext[x, y, z] = tile

    row = lax.broadcasted_iota(jnp.int32, (8, width), 0)
    low, top = row % 4, row < 4
    center = [0.5 * size for size in ext_sizes]
    wide_row = lax.broadcasted_iota(jnp.int32, (32, 4 * width), 0)
    wide_axis = lax.broadcasted_iota(jnp.int32, (32, 4 * width), 1) // width
    picked = (wide_row == wide_axis) | (wide_row == wide_axis + 8) | (wide_row == wide_axis + 20)
    picked = jnp.where(picked & (wide_axis < 3), 1.0, 0.0)
    picked = jnp.where((wide_axis == 3) & (wide_row == 27), 1.0, picked)
    pick[...] = picked.astype(jnp.bfloat16)

    def build(some):
        for x, y, z in some:
            cell = index_of(x, y, z)
            base = jnp.where(low == 0, x - center[0], jnp.where(low == 1, y - center[1], z - center[2]))
            lines = ext[x, y, z]
            rows[pl.ds(row_of[x, y, z], 1)] = lines[3:4]
            both = jnp.concatenate([lines, lines], 0)
            live = jnp.broadcast_to(lines[3:4], (8, width)) >= 0.0
            place = jnp.where(live & (low < 3), both + base, 0.0)
            for axis in range(3):
                table[cell, axis] = jnp.broadcast_to(place[axis : axis + 1], (8, width))
            norm = jnp.sum((place * place)[0:4], 0, keepdims=True)
            norm = jnp.where(live, jnp.broadcast_to(norm, (8, width)), far)
            high, mid, tiny = split(jnp.where(low == 3, norm, place))
            twice, twice_mid, twice_tiny = split(jnp.where(low == 3, norm + soft_core, -2.0 * place))
            high_one = jnp.where(row == 3, 1.0, high)
            twice_one = jnp.where(row == 3, 1.0, twice)
            right[cell] = jnp.concatenate(
                [
                    jnp.where(top, twice_one, jnp.where(row == 7, twice, twice_mid)),
                    jnp.where(top, twice_one, twice_mid),
                    jnp.where(top, twice_tiny, jnp.where(row == 7, 1.0, twice)),
                    jnp.zeros((8, width), jnp.float32),
                ],
                0,
            ).astype(jnp.bfloat16)
            if outside((x, y, z)) <= 1:
                turned = jnp.transpose(
                    jnp.concatenate(
                        [
                            jnp.where(row == 7, 1.0, high),
                            jnp.where(row == 7, 1.0, mid),
                            jnp.where(top, high_one, tiny),
                            both,
                        ],
                        0,
                    )
                )
                turned = turned.astype(jnp.bfloat16)
                left[cell] = turned
                spread = jnp.dot(turned, pick[...], preferred_element_type=jnp.float32)
                for axis in range(4):
                    first[cell, axis] = spread[:, axis * width : (axis + 1) * width].reshape(
                        (groups, 8, width)
                    )
            kind_row = jnp.broadcast_to(lines[3:4], (8, width))
            same = [kind_row == float(kind) for kind in range(types)]
            for kind in range(1, types):
                total = jnp.sum(same[kind].astype(jnp.float32), 1, keepdims=True) * 0.125
                number_of[cell, kind - 1] = jnp.broadcast_to(total, (8, width))
            for kind in range(types):
                for at in range(5):
                    picked = jnp.zeros((8, width), jnp.float32)
                    for second_kind in range(types):
                        picked = jnp.where(same[second_kind], tables[kind, second_kind][at], picked)
                    table[cell, 3 + 5 * kind + at] = picked

    build(inner)

    def interact(own_at, other, kinds, soft_sq, ordered=None):
        xi, yi, zi = own_at
        second = [table[other, at][None] for at in range(per_cell)]

        def chosen(at):
            value = second[3 + at]
            for kind in range(1, types):
                value = jnp.where(kinds[kind - 1], second[3 + 5 * kind + at], value)
            return value

        dx, dy, dz = second[0] - xi, second[1] - yi, second[2] - zi
        soft_sq = jnp.minimum(soft_sq, cut_sq)
        inverse = lax.rsqrt(soft_sq)
        inverse_2 = inverse * inverse
        inverse_6 = inverse_2 * inverse_2 * inverse_2
        twelve = chosen(0) * inverse_6 * inverse_6
        six = chosen(1) * inverse_6
        coulomb = chosen(2) * inverse
        shift = chosen(3) * (soft_sq * inverse)
        drive = (six - twelve) - (coulomb + shift)
        slope = drive * inverse_2
        forces = (slope * dx, slope * dy, slope * dz)
        for axis in range(3):
            force_j[other, axis] -= jnp.sum(forces[axis], 0)
        if ordered is None:
            terms = (twelve, six, coulomb, shift, slope)
            return forces, [jnp.sum(term, 0) for term in terms]
        value = twelve * (1.0 / 12.0) - six * (1.0 / 6.0) + coulomb - shift + chosen(4)
        pull = drive - soft_core * slope
        return [jnp.sum(jnp.where(ordered, term, 0.0), 0) for term in (value, pull)]

    def slots(depth):
        shape = (depth, 8, width)
        return (
            lax.broadcasted_iota(jnp.int32, shape, 0) * 8
            + lax.broadcasted_iota(jnp.int32, shape, 1)
            - lax.broadcasted_iota(jnp.int32, shape, 2)
        )

    def load_first(here, span):
        own_at = tuple(first[here, axis, span] for axis in range(3))
        kind_at = first[here, 3, span]
        return own_at, [kind_at == float(kind) for kind in range(1, types)]

    def alone(here, held, sums):
        slot_at = slots(4)
        for start in range(0, groups, 4):
            span = pl.ds(start, 4)
            own_at, kinds = load_first(here, span)
            values = interact(
                own_at, here, kinds, held[0, span], ordered=slot_at + start * 8 < 0
            )
            sums = tuple(a + b for a, b in zip(sums, values))
        return sums

    def apart(store, here):
        found = jnp.dot(left[here], right[here], preferred_element_type=jnp.float32)
        store[0] = found.reshape((groups, 8, width))

    def levels(energy, here, others):
        numbers = [number_of[here, kind - 1] for kind in range(1, types)]
        rest = jnp.full((8, width), float(groups))
        for number in numbers:
            rest = rest - number
        for other in others:
            for kind, number in enumerate([rest, *numbers]):
                energy = energy + number * table[other, 3 + 5 * kind + 4]
        return energy

    roles = {
        first_corner: tuple(which for which in seconds if which)
        for first_corner, seconds in second_of.items()
    }
    depth = 4
    trips = groups // depth
    offset_of = {}
    for first_corner, seconds in roles.items():
        offset_of[first_corner] = sum(len(roles[corner]) for corner in offset_of)

    def distances(store, cell_at, chunk, first_corner):
        wide = 8 * depth
        lefts = left[cell_at(first_corner), pl.ds(chunk * wide, wide)]
        seconds = roles[first_corner]
        for at in range(0, len(seconds), 2):
            some = [right[cell_at(which)] for which in seconds[at : at + 2]]
            found = jnp.dot(
                lefts,
                jnp.concatenate(some, 1) if len(some) > 1 else some[0],
                preferred_element_type=jnp.float32,
            )
            for n in range(len(some)):
                store[offset_of[first_corner] + at + n, pl.ds(chunk * depth, depth)] = found[:, n * width : (n + 1) * width].reshape(
                    (depth, 8, width)
                )

    def role(first_corner, member, cell_at, chunk, held, sums):
        here = cell_at(first_corner)
        part_at = tuple(second_of).index(first_corner)
        fine = 4 if first_corner == 0 else 4
        for start in range(0, depth, fine):
            span = pl.ds(chunk * depth + start, fine)
            own_at, kinds = load_first(here, span)
            total = None
            parts = None
            for n, which in enumerate(roles[first_corner]):
                forces, terms = interact(
                    own_at,
                    cell_at(which),
                    kinds,
                    held[offset_of[first_corner] + n, pl.ds(chunk * depth + start, fine)],
                )
                parts = terms if parts is None else [a + b for a, b in zip(parts, terms)]
                total = forces if total is None else [a + b for a, b in zip(total, forces)]
            twelve, six, coulomb, shift, slope = parts
            value = (twelve * (1.0 / 12.0) - six * (1.0 / 6.0)) + (coulomb - shift)
            pull = ((six - twelve) - (coulomb + shift)) - soft_core * slope
            for axis in range(3):
                force_i[part_at, member, axis, span] = total[axis]
            sums = sums[0] + value, sums[1] + pull
        return sums

    def corners(x0, y0, z0):
        def cell_at(which):
            shift = corner_of(which)
            return index_of(x0 + shift[0], y0 + shift[1], z0 + shift[2])

        return cell_at

    def one_pair(at, sums):
        cell = [
            index_of(
                member // (sizes[2] * sizes[1]),
                lax.rem(member // sizes[2], sizes[1]),
                lax.rem(member, sizes[2]),
            )
            for member in (2 * at, 2 * at + 1, jnp.minimum(2 * at + 2, members - 1))
        ]
        apart(odd, cell[1])
        sums = alone(cell[0], even, sums)
        apart(even, cell[2])
        return alone(cell[1], odd, sums)

    def across(homes, sums):
        stores = (even, odd)
        for first_corner in roles:
            for chunk in range(trips):
                distances(even, corners(*homes[0]), chunk, first_corner)
        for at, (x0, y0, z0) in enumerate(homes):
            member = (x0 * sizes[1] + y0) * sizes[2] + z0
            cell_at = corners(x0, y0, z0)
            held, store = stores[at % 2], stores[(at + 1) % 2]
            after = corners(*homes[at + 1]) if at + 1 < len(homes) else None

            def step(chunk, sums, some):
                for first_corner in some:
                    if after is not None:
                        distances(store, after, chunk, first_corner)
                for first_corner in some:
                    sums = role(first_corner, member, cell_at, chunk, held, sums)
                return sums

            for some in ((0,), tuple(corner for corner in roles if corner)):
                sums = lax.fori_loop(0, trips, functools.partial(step, some=some), sums)
        return sums

    blank = jnp.zeros((8, width), jnp.float32)
    apart(even, index_of(0, 0, 0))
    sums = lax.fori_loop(0, members // 2, one_pair, (blank, blank))

    def base_level(member, energy):
        z0 = lax.rem(member, sizes[2])
        y0 = lax.rem(member // sizes[2], sizes[1])
        x0 = member // (sizes[2] * sizes[1])
        cell_at = corners(x0, y0, z0)
        for first_corner, seconds in roles.items():
            energy = levels(energy, cell_at(first_corner), [cell_at(which) for which in seconds])
        return energy


    pl.semaphore_wait(barrier, greeted)
    halos = []
    for which in range(1, 8):
        bits = corner_of(which)
        source = tuple(pl.ds(0, 1 if bit else size) for bit, size in zip(bits, sizes))
        target = tuple(
            pl.ds(size, 1) if bit else pl.ds(0, size) for bit, size in zip(bits, sizes)
        )
        copy = pltpu.make_async_remote_copy(
            src_ref=own.at[source],
            dst_ref=ext.at[target],
            send_sem=halo_send.at[which],
            recv_sem=halo_recv.at[which],
            device_id=neighbour(which, -1),
            device_id_type=MESH,
        )
        copy.start()
        halos.append(copy)

    less = tuple(size - 1 for size in sizes)

    homes = [
        (x, y, z) for x in range(sizes[0]) for y in range(sizes[1]) for z in range(sizes[2])
    ]
    inside = [home for home in homes if all(at < most for at, most in zip(home, less))]
    sheet = [home for home in homes if home[0] == less[0]]
    border = [home for home in homes if home not in inside and home not in sheet]
    if inside:
        sums = across(inside, sums)

    for copy in halos:
        copy.wait()
    build(outer)

    def reduced(cell):
        x, y, z = cell
        at_cell = index_of(x, y, z)
        held = rows[pl.ds(row_of[cell], 1)] >= 0.0
        lines = []
        for axis in range(3):
            line = force_j[at_cell, axis]
            partial = None
            for part_at, first_corner in enumerate(second_of):
                spot = [at - bit for at, bit in zip(cell, corner_of(first_corner))]
                if all(0 <= at < size for at, size in zip(spot, sizes)):
                    member = (spot[0] * sizes[1] + spot[1]) * sizes[2] + spot[2]
                    value = force_i[part_at, member, axis].reshape((width, width))
                    partial = value if partial is None else partial + value
            if partial is not None:
                turned = jnp.transpose(partial)
                line = line + jnp.sum(turned.reshape((groups, 8, width)), 0)
            line = jnp.sum(line, 0, keepdims=True)
            lines.append(jnp.where(held, line, 0.0))
        return jnp.concatenate(lines, 0)

    backs = []

    def give_back(some):
        for cell in outer:
            which = sum((at == size) << bit for bit, (at, size) in enumerate(zip(cell, sizes)))
            if which in some:
                react[cell[0], cell[1], cell[2], 0:3] = reduced(cell)
        for which in some:
            source = tuple(
                pl.ds(size, 1) if bit else pl.ds(0, size)
                for bit, size in zip(corner_of(which), sizes)
            )
            copy = pltpu.make_async_remote_copy(
                src_ref=react.at[source],
                dst_ref=landed[which - 1],
                send_sem=back_send.at[which],
                recv_sem=back_recv.at[which],
                device_id=neighbour(which, 1),
                device_id_type=MESH,
            )
            copy.start()
            backs.append(copy)

    sums = across(sheet, sums)
    give_back((1, 3, 5, 7))
    energy = lax.fori_loop(0, members, base_level, sums[0])
    sums = energy, sums[1]
    if border:
        sums = across(border, sums)
    part[0:1] = jnp.sum(sums[0], 0, keepdims=True)
    part[1:2] = jnp.sum(sums[1], 0, keepdims=True)

    def send_plane():
        plane_copies = []
        for step in range(1, count_plane):
            copy = pltpu.make_async_remote_copy(
                src_ref=part if direct else middle,
                dst_ref=plane.at[at_plane],
                send_sem=plane_send.at[step],
                recv_sem=plane_recv.at[step],
                device_id=plane_target(step),
                device_id_type=MESH,
            )
            copy.start()
            plane_copies.append(copy)
        return plane_copies

    if direct:
        plane_copies = send_plane()
        plane[at_plane] = part[...]
    else:
        line_copies = []
        for step in range(1, count_x):
            copy = pltpu.make_async_remote_copy(
                src_ref=part,
                dst_ref=line.at[at_x],
                send_sem=line_send.at[step],
                recv_sem=line_recv.at[step],
                device_id=line_target(step),
                device_id_type=MESH,
            )
            copy.start()
            line_copies.append(copy)
        line[at_x] = part[...]
        for copy in line_copies:
            copy.wait()
        summed = line[0]
        for step in range(1, count_x):
            summed = summed + line[step]
        middle[...] = summed
        plane[at_plane] = summed
        plane_copies = send_plane()
    give_back((2, 4, 6))
    for cell in inner:
        react[cell[0], cell[1], cell[2], 0:3] = reduced(cell)
    for copy in backs:
        copy.wait()
    for x, y, z in inner:
        value = react[x, y, z]
        for which in range(1, 8):
            bits = corner_of(which)
            spot = (x, y, z)
            if all(not bit or at == 0 for bit, at in zip(bits, spot)):
                value = value + landed[which - 1][
                    tuple(0 if bit else at for bit, at in zip(bits, spot))
                ]
        for axis in range(3):
            at = ((axis * sizes[0] + x) * sizes[1] + y) * sizes[2] + z
            forces[pl.ds(at, 1)] = value[axis : axis + 1]
    for copy in plane_copies:
        copy.wait()
    summed = plane[0]
    for step in range(1, count_plane):
        summed = summed + plane[step]
    totals[0] = jnp.sum(summed[0:1]) * normaliser
    totals[1] = jnp.sum(summed[1:2]) * normaliser


def per_device(positions, type_ids, counts, type_charge, type_sigma, type_epsilon):
    types = type_charge.shape[0]
    sizes, width = type_ids.shape[:3], type_ids.shape[3]
    ext_sizes = tuple(size + 1 for size in sizes)
    cells = ext_sizes[0] * ext_sizes[1] * ext_sizes[2]
    members = sizes[0] * sizes[1] * sizes[2]
    vmem = pl.BlockSpec(memory_space=pltpu.VMEM)
    smem = pl.BlockSpec(memory_space=pltpu.SMEM)
    hbm = pl.BlockSpec(memory_space=pltpu.HBM)
    f32 = jnp.float32
    count_x, count_y, count_z = (lax.axis_size(axis) for axis in AXES)
    count_plane = count_y * count_z
    slots_x, slots_plane = count_x, count_plane
    if count_x * count_plane <= direct_limit:
        slots_x, slots_plane = 1, count_x * count_plane
    normaliser = 1.0 / (
        sizes[0] * count_x * sizes[1] * count_y * sizes[2] * count_z * width
    )
    landing = [
        pltpu.VMEM(
            tuple(1 if bit else size for bit, size in zip(corner_of(which), sizes)) + (4, width),
            f32,
        )
        for which in range(1, 8)
    ]
    counts = jnp.transpose(counts, (0, 2, 1))
    positions, type_ids, counts = (
        pltpu.with_memory_space_constraint(value, pltpu.HBM) for value in (positions, type_ids, counts)
    )
    type_charge, type_sigma, type_epsilon = (
        pltpu.with_memory_space_constraint(value, pltpu.HBM)
        for value in (type_charge, type_sigma, type_epsilon)
    )
    dma = pltpu.SemaphoreType.DMA
    forces, totals = pl.pallas_call(
        functools.partial(step_kernel, normaliser, types),
        name="step",
        out_shape=(
            jax.ShapeDtypeStruct((3 * members, width), f32),
            jax.ShapeDtypeStruct((2,), f32),
        ),
        in_specs=[smem, smem, smem, hbm, hbm, hbm],
        out_specs=(vmem, smem),
        scratch_shapes=[
            pltpu.VMEM(positions.shape, f32),
            pltpu.VMEM(type_ids.shape, jnp.int32),
            pltpu.VMEM(counts.shape, jnp.int32),
            pltpu.VMEM(sizes + (4, width), f32),
            pltpu.VMEM(ext_sizes + (4, width), f32),
            pltpu.VMEM((cells, width), f32),
            pltpu.VMEM((32, 4 * width), jnp.bfloat16),
            pltpu.VMEM((cells, width, 32), jnp.bfloat16),
            pltpu.VMEM((cells, 32, width), jnp.bfloat16),
            pltpu.VMEM((13, width // 8, 8, width), f32),
            pltpu.VMEM((13, width // 8, 8, width), f32),
            pltpu.VMEM((cells, 4, width // 8, 8, width), f32),
            pltpu.VMEM((cells, 3 + 5 * types, 8, width), f32),
            pltpu.VMEM((cells, types - 1, 8, width), f32),
            pltpu.VMEM((len(second_of), members, 3, width // 8, 8, width), f32),
            pltpu.VMEM((cells, 3, 8, width), f32),
            pltpu.VMEM(ext_sizes + (4, width), f32),
            pltpu.VMEM((2, width), f32),
            dma((3,)),
            dma((8,)),
            dma((8,)),
            dma((8,)),
            dma((8,)),
            pltpu.VMEM((slots_x, 2, width), f32),
            pltpu.VMEM((slots_plane, 2, width), f32),
            pltpu.VMEM((2, width), f32),
            dma((slots_x,)),
            dma((slots_x,)),
            dma((slots_plane,)),
            dma((slots_plane,)),
        ]
        + landing,
        compiler_params=pltpu.CompilerParams(
            collective_id=0, has_side_effects=True, vmem_limit_bytes=VMEM_LIMIT
        ),
    )(type_charge, type_sigma, type_epsilon, positions, type_ids, counts)
    return forces.reshape((3,) + sizes + (width,)), totals


def solution(mesh):
    in_specs = (
        P(None, "gx", "gy", "gz", None),
        P("gx", "gy", "gz", None),
        P("gx", "gy", "gz"),
        P(),
        P(),
        P(),
    )
    out_specs = (P(None, "gx", "gy", "gz", None), P())
    return jax.shard_map(
        per_device, mesh=mesh, in_specs=in_specs, out_specs=out_specs, check_vma=False
    )
```

```python
import functools

import jax
import jax.numpy as jnp
from jax import lax
from jax.experimental import pallas as pl
from jax.experimental.pallas import tpu as pltpu
from jax.sharding import PartitionSpec as P

MESH = pl.DeviceIdType.MESH
AXES = ("gx", "gy", "gz")
soft_core = 0.09
cut_sq = 1.0 + soft_core
cut_len = cut_sq**0.5
second_of = {0: (0, 1, 2, 3, 4, 5, 6, 7), 1: (2, 6), 2: (4, 5), 4: (1, 3)}
direct_limit = 64
far = 1024.0
VMEM_LIMIT = 40 * 1024 * 1024


def corner_of(which):
    return (which & 1, which >> 1 & 1, which >> 2 & 1)


def neighbour(which, step):
    target = {}
    for axis, bit in zip(AXES, corner_of(which)):
        if bit:
            count = lax.axis_size(axis)
            target[axis] = lax.rem(lax.axis_index(axis) + step + count, count)
    return target


def split(value):
    high = value.astype(jnp.bfloat16).astype(jnp.float32)
    rest = value - high
    middle = rest.astype(jnp.bfloat16).astype(jnp.float32)
    return high, middle, rest - middle


def type_tables(types, shape, charges, sigmas, epsilons):
    def full(value):
        return jnp.full(shape, value, jnp.float32)

    charge = [full(charges[kind]) for kind in range(types)]
    sigma = [full(sigmas[kind]) for kind in range(types)]
    root = [jnp.sqrt(full(epsilons[kind])) for kind in range(types)]
    tables = {}
    for a in range(types):
        for b in range(types):
            sigma_pair = 0.5 * (sigma[a] + sigma[b])
            depth_pair = 4.0 * root[a] * root[b]
            coulomb = charge[a] * charge[b]
            square = sigma_pair * sigma_pair
            sig_six = square * square * square
            six = 6.0 * depth_pair * sig_six
            twelve = 12.0 * depth_pair * sig_six * sig_six
            cut_six, cut_twelve, cut_coulomb = six * cut_sq**-3, twelve * cut_sq**-6, coulomb / cut_len
            shift = ((cut_six - cut_twelve) - cut_coulomb) / cut_len
            level = cut_len * shift - (cut_twelve / 12.0 - cut_six / 6.0 + cut_coulomb)
            tables[a, b] = (twelve, six, coulomb, shift, level)
    return tables


def step_kernel(
    normaliser, types, charges, sigmas, epsilons, positions, type_ids, counts, forces, totals,
    place_in, kind_in, count_in, own, ext, rows, pick, left, right, even, odd, first, table, number_of, force_i, force_j, react, part,
    in_sem, halo_send, halo_recv, back_send, back_recv,
    line, plane, middle, line_send, line_recv, plane_send, plane_recv, *landed,
):
    sizes = own.shape[:3]
    ext_sizes = ext.shape[:3]
    width = own.shape[-1]
    groups = width // 8
    per_cell = 3 + 5 * types
    members = sizes[0] * sizes[1] * sizes[2]
    count_x, count_y, count_z = (lax.axis_size(axis) for axis in AXES)
    at_x, at_y, at_z = (lax.axis_index(axis) for axis in AXES)
    count_plane = count_y * count_z
    at_plane = at_y * count_z + at_z
    direct = count_x * count_plane <= direct_limit
    loads = [
        pltpu.make_async_copy(source, target, in_sem.at[at])
        for at, (source, target) in enumerate(
            ((positions, place_in), (type_ids, kind_in), (counts, count_in))
        )
    ]
    for load in loads:
        load.start()

    def around(at, count):
        return [at] + [at + step - count * (at + step >= count).astype(jnp.int32) for step in range(1, count)]

    spots = [around(at, count) for at, count in ((at_x, count_x), (at_y, count_y), (at_z, count_z))]
    if direct:
        count_plane, at_plane = count_x * count_plane, at_x * count_plane + at_plane
        count_x, at_x = 1, 0

    def line_target(step):
        return {"gx": spots[0][step]}

    def plane_target(step):
        target = {"gy": spots[1][step // count_z % count_y], "gz": spots[2][step % count_z]}
        if direct:
            target["gx"] = spots[0][step // (count_y * count_z)]
        return target

    barrier = pltpu.get_barrier_semaphore()
    greeted = count_x - 1 + count_plane - 1
    if not direct:
        greeted += 14
        for which in range(1, 8):
            for step in (1, -1):
                pl.semaphore_signal(barrier, inc=1, device_id=neighbour(which, step), device_id_type=MESH)
    for step in range(1, count_x):
        pl.semaphore_signal(barrier, inc=1, device_id=line_target(step), device_id_type=MESH)
    for step in range(1, count_plane):
        pl.semaphore_signal(barrier, inc=1, device_id=plane_target(step), device_id_type=MESH)

    cells = [
        (x, y, z)
        for x in range(ext_sizes[0])
        for y in range(ext_sizes[1])
        for z in range(ext_sizes[2])
    ]

    def outside(cell):
        return sum(at == size for at, size in zip(cell, sizes))

    def index_of(x, y, z):
        return (x * ext_sizes[1] + y) * ext_sizes[2] + z

    ordered = sorted(cells, key=outside)
    row_of = {cell: at for at, cell in enumerate(ordered)}
    inner = [cell for cell in ordered if outside(cell) == 0]
    outer = [cell for cell in ordered if outside(cell) > 0]

    tables = type_tables(types, (8, width), charges, sigmas, epsilons)
    force_j[...] = jnp.zeros(force_j.shape, jnp.float32)
    react[...] = jnp.zeros(react.shape, jnp.float32)
    slot = lax.broadcasted_iota(jnp.int32, (1, width), 1)

    for load in loads:
        load.wait()
    for x, y, z in inner:
        lines = [place_in[axis, x, y, pl.ds(z, 1)] for axis in range(3)]
        kind = kind_in[x, y, pl.ds(z, 1)].astype(jnp.float32)
        held = jnp.broadcast_to(count_in[x, pl.ds(z, 1), pl.ds(y, 1)], (1, width))
        lines.append(jnp.where(slot < held, kind, -1.0))
        tile = jnp.concatenate(lines, 0)
        own[x, y, z] = tile
        ext[x, y, z] = tile

    row = lax.broadcasted_iota(jnp.int32, (8, width), 0)
    low, top = row % 4, row < 4
    center = [0.5 * size for size in ext_sizes]
    wide_row = lax.broadcasted_iota(jnp.int32, (32, 4 * width), 0)
    wide_axis = lax.broadcasted_iota(jnp.int32, (32, 4 * width), 1) // width
    picked = (wide_row == wide_axis) | (wide_row == wide_axis + 8) | (wide_row == wide_axis + 20)
    picked = jnp.where(picked & (wide_axis < 3), 1.0, 0.0)
    picked = jnp.where((wide_axis == 3) & (wide_row == 27), 1.0, picked)
    pick[...] = picked.astype(jnp.bfloat16)

    def build(some):
        for x, y, z in some:
            cell = index_of(x, y, z)
            base = jnp.where(low == 0, x - center[0], jnp.where(low == 1, y - center[1], z - center[2]))
            lines = ext[x, y, z]
            rows[pl.ds(row_of[x, y, z], 1)] = lines[3:4]
            both = jnp.concatenate([lines, lines], 0)
            live = jnp.broadcast_to(lines[3:4], (8, width)) >= 0.0
            place = jnp.where(live & (low < 3), both + base, 0.0)
            for axis in range(3):
                table[cell, axis] = jnp.broadcast_to(place[axis : axis + 1], (8, width))
            norm = jnp.sum((place * place)[0:4], 0, keepdims=True)
            norm = jnp.where(live, jnp.broadcast_to(norm, (8, width)), far)
            high, mid, tiny = split(jnp.where(low == 3, norm, place))
            twice, twice_mid, twice_tiny = split(jnp.where(low == 3, norm + soft_core, -2.0 * place))
            high_one = jnp.where(row == 3, 1.0, high)
            twice_one = jnp.where(row == 3, 1.0, twice)
            right[cell] = jnp.concatenate(
                [
                    jnp.where(top, twice_one, jnp.where(row == 7, twice, twice_mid)),
                    jnp.where(top, twice_one, twice_mid),
                    jnp.where(top, twice_tiny, jnp.where(row == 7, 1.0, twice)),
                    jnp.zeros((8, width), jnp.float32),
                ],
                0,
            ).astype(jnp.bfloat16)
            if outside((x, y, z)) <= 1:
                turned = jnp.transpose(
                    jnp.concatenate(
                        [
                            jnp.where(row == 7, 1.0, high),
                            jnp.where(row == 7, 1.0, mid),
                            jnp.where(top, high_one, tiny),
                            both,
                        ],
                        0,
                    )
                )
                turned = turned.astype(jnp.bfloat16)
                left[cell] = turned
                spread = jnp.dot(turned, pick[...], preferred_element_type=jnp.float32)
                for axis in range(4):
                    first[cell, axis] = spread[:, axis * width : (axis + 1) * width].reshape(
                        (groups, 8, width)
                    )
            kind_row = jnp.broadcast_to(lines[3:4], (8, width))
            same = [kind_row == float(kind) for kind in range(types)]
            for kind in range(1, types):
                total = jnp.sum(same[kind].astype(jnp.float32), 1, keepdims=True) * 0.125
                number_of[cell, kind - 1] = jnp.broadcast_to(total, (8, width))
            for kind in range(types):
                for at in range(5):
                    picked = jnp.zeros((8, width), jnp.float32)
                    for second_kind in range(types):
                        picked = jnp.where(same[second_kind], tables[kind, second_kind][at], picked)
                    table[cell, 3 + 5 * kind + at] = picked

    build(inner)

    def interact(own_at, other, kinds, soft_sq, ordered=None):
        xi, yi, zi = own_at
        second = [table[other, at][None] for at in range(per_cell)]

        def chosen(at):
            value = second[3 + at]
            for kind in range(1, types):
                value = jnp.where(kinds[kind - 1], second[3 + 5 * kind + at], value)
            return value

        dx, dy, dz = second[0] - xi, second[1] - yi, second[2] - zi
        soft_sq = jnp.minimum(soft_sq, cut_sq)
        inverse = lax.rsqrt(soft_sq)
        inverse_2 = inverse * inverse
        inverse_6 = inverse_2 * inverse_2 * inverse_2
        twelve = chosen(0) * inverse_6 * inverse_6
        six = chosen(1) * inverse_6
        coulomb = chosen(2) * inverse
        shift = chosen(3) * (soft_sq * inverse)
        drive = (six - twelve) - (coulomb + shift)
        slope = drive * inverse_2
        forces = (slope * dx, slope * dy, slope * dz)
        for axis in range(3):
            force_j[other, axis] -= jnp.sum(forces[axis], 0)
        if ordered is None:
            terms = (twelve, six, coulomb, shift, slope)
            return forces, [jnp.sum(term, 0) for term in terms]
        value = twelve * (1.0 / 12.0) - six * (1.0 / 6.0) + coulomb - shift + chosen(4)
        pull = drive - soft_core * slope
        return [jnp.sum(jnp.where(ordered, term, 0.0), 0) for term in (value, pull)]

    def slots(depth):
        shape = (depth, 8, width)
        return (
            lax.broadcasted_iota(jnp.int32, shape, 0) * 8
            + lax.broadcasted_iota(jnp.int32, shape, 1)
            - lax.broadcasted_iota(jnp.int32, shape, 2)
        )

    def load_first(here, span):
        own_at = tuple(first[here, axis, span] for axis in range(3))
        kind_at = first[here, 3, span]
        return own_at, [kind_at == float(kind) for kind in range(1, types)]

    def alone(here, held, sums):
        slot_at = slots(4)
        for start in range(0, groups, 4):
            span = pl.ds(start, 4)
            own_at, kinds = load_first(here, span)
            values = interact(
                own_at, here, kinds, held[0, span], ordered=slot_at + start * 8 < 0
            )
            sums = tuple(a + b for a, b in zip(sums, values))
        return sums

    def apart(store, here):
        found = jnp.dot(left[here], right[here], preferred_element_type=jnp.float32)
        store[0] = found.reshape((groups, 8, width))

    def levels(energy, here, others):
        numbers = [number_of[here, kind - 1] for kind in range(1, types)]
        rest = jnp.full((8, width), float(groups))
        for number in numbers:
            rest = rest - number
        for other in others:
            for kind, number in enumerate([rest, *numbers]):
                energy = energy + number * table[other, 3 + 5 * kind + 4]
        return energy

    roles = {
        first_corner: tuple(which for which in seconds if which)
        for first_corner, seconds in second_of.items()
    }
    depth = 4
    trips = groups // depth
    offset_of = {}
    for first_corner, seconds in roles.items():
        offset_of[first_corner] = sum(len(roles[corner]) for corner in offset_of)

    def distances(store, cell_at, chunk, first_corner):
        wide = 8 * depth
        lefts = left[cell_at(first_corner), pl.ds(chunk * wide, wide)]
        seconds = roles[first_corner]
        for at in range(0, len(seconds), 2):
            some = [right[cell_at(which)] for which in seconds[at : at + 2]]
            found = jnp.dot(
                lefts,
                jnp.concatenate(some, 1) if len(some) > 1 else some[0],
                preferred_element_type=jnp.float32,
            )
            for n in range(len(some)):
                store[offset_of[first_corner] + at + n, pl.ds(chunk * depth, depth)] = found[:, n * width : (n + 1) * width].reshape(
                    (depth, 8, width)
                )

    def role(first_corner, member, cell_at, chunk, held, sums):
        here = cell_at(first_corner)
        part_at = tuple(second_of).index(first_corner)
        fine = 4 if first_corner == 0 else 4
        for start in range(0, depth, fine):
            span = pl.ds(chunk * depth + start, fine)
            own_at, kinds = load_first(here, span)
            total = None
            parts = None
            for n, which in enumerate(roles[first_corner]):
                forces, terms = interact(
                    own_at,
                    cell_at(which),
                    kinds,
                    held[offset_of[first_corner] + n, pl.ds(chunk * depth + start, fine)],
                )
                parts = terms if parts is None else [a + b for a, b in zip(parts, terms)]
                total = forces if total is None else [a + b for a, b in zip(total, forces)]
            twelve, six, coulomb, shift, slope = parts
            value = (twelve * (1.0 / 12.0) - six * (1.0 / 6.0)) + (coulomb - shift)
            pull = ((six - twelve) - (coulomb + shift)) - soft_core * slope
            for axis in range(3):
                force_i[part_at, member, axis, span] = total[axis]
            sums = sums[0] + value, sums[1] + pull
        return sums

    def corners(x0, y0, z0):
        def cell_at(which):
            shift = corner_of(which)
            return index_of(x0 + shift[0], y0 + shift[1], z0 + shift[2])

        return cell_at

    def one_pair(at, sums):
        cell = [
            index_of(
                member // (sizes[2] * sizes[1]),
                lax.rem(member // sizes[2], sizes[1]),
                lax.rem(member, sizes[2]),
            )
            for member in (2 * at, 2 * at + 1, jnp.minimum(2 * at + 2, members - 1))
        ]
        apart(odd, cell[1])
        sums = alone(cell[0], even, sums)
        apart(even, cell[2])
        return alone(cell[1], odd, sums)

    def across(count, locate, sums):
        def one_home(home, after, held, store, sums):
            x0, y0, z0 = home
            member = (x0 * sizes[1] + y0) * sizes[2] + z0
            cell_at = corners(x0, y0, z0)
            after_at = None if after is None else corners(*after)

            def step(chunk, sums, some):
                for first_corner in some:
                    if after is not None:
                        distances(store, after_at, chunk, first_corner)
                for first_corner in some:
                    sums = role(first_corner, member, cell_at, chunk, held, sums)
                return sums

            for some in ((0,), tuple(corner for corner in roles if corner)):
                sums = lax.fori_loop(0, trips, functools.partial(step, some=some), sums)
            return sums

        def two_homes(at, sums):
            spot = 2 * at
            sums = one_home(locate(spot), locate(spot + 1), even, odd, sums)
            after = locate(jnp.minimum(spot + 2, count - 1))
            return one_home(locate(spot + 1), after, odd, even, sums)

        cell_at = corners(*locate(0))
        for first_corner in roles:
            for chunk in range(trips):
                distances(even, cell_at, chunk, first_corner)
        sums = lax.fori_loop(0, count // 2, two_homes, sums)
        if count % 2:
            sums = one_home(locate(count - 1), None, even, odd, sums)
        return sums

    blank = jnp.zeros((8, width), jnp.float32)
    apart(even, index_of(0, 0, 0))
    sums = lax.fori_loop(0, members // 2, one_pair, (blank, blank))

    def base_level(member, energy):
        z0 = lax.rem(member, sizes[2])
        y0 = lax.rem(member // sizes[2], sizes[1])
        x0 = member // (sizes[2] * sizes[1])
        cell_at = corners(x0, y0, z0)
        for first_corner, seconds in roles.items():
            energy = levels(energy, cell_at(first_corner), [cell_at(which) for which in seconds])
        return energy


    pl.semaphore_wait(barrier, greeted)
    halos = []
    for which in range(1, 8):
        bits = corner_of(which)
        source = tuple(pl.ds(0, 1 if bit else size) for bit, size in zip(bits, sizes))
        target = tuple(
            pl.ds(size, 1) if bit else pl.ds(0, size) for bit, size in zip(bits, sizes)
        )
        copy = pltpu.make_async_remote_copy(
            src_ref=own.at[source],
            dst_ref=ext.at[target],
            send_sem=halo_send.at[which],
            recv_sem=halo_recv.at[which],
            device_id=neighbour(which, -1),
            device_id_type=MESH,
        )
        copy.start()
        halos.append(copy)

    less = tuple(size - 1 for size in sizes)

    def inside(at):
        return at // (less[2] * less[1]), lax.rem(at // less[2], less[1]), lax.rem(at, less[2])

    def sheet(at):
        return less[0], at // sizes[2], lax.rem(at, sizes[2])

    def border(at):
        on_bar = at < bar
        rest = at - bar
        x0 = jnp.where(on_bar, at // sizes[2], rest // max(less[1], 1))
        y0 = jnp.where(on_bar, less[1], lax.rem(rest, max(less[1], 1)))
        z0 = jnp.where(on_bar, lax.rem(at, sizes[2]), less[2])
        return x0, y0, z0

    bar = less[0] * sizes[2]
    if less[0] * less[1] * less[2]:
        sums = across(less[0] * less[1] * less[2], inside, sums)

    for copy in halos:
        copy.wait()
    build(outer)

    def reduced(cell):
        x, y, z = cell
        at_cell = index_of(x, y, z)
        held = rows[pl.ds(row_of[cell], 1)] >= 0.0
        lines = []
        for axis in range(3):
            line = force_j[at_cell, axis]
            partial = None
            for part_at, first_corner in enumerate(second_of):
                spot = [at - bit for at, bit in zip(cell, corner_of(first_corner))]
                if all(0 <= at < size for at, size in zip(spot, sizes)):
                    member = (spot[0] * sizes[1] + spot[1]) * sizes[2] + spot[2]
                    value = force_i[part_at, member, axis].reshape((width, width))
                    partial = value if partial is None else partial + value
            if partial is not None:
                turned = jnp.transpose(partial)
                line = line + jnp.sum(turned.reshape((groups, 8, width)), 0)
            line = jnp.sum(line, 0, keepdims=True)
            lines.append(jnp.where(held, line, 0.0))
        return jnp.concatenate(lines, 0)

    backs = []

    def give_back(some):
        for cell in outer:
            which = sum((at == size) << bit for bit, (at, size) in enumerate(zip(cell, sizes)))
            if which in some:
                react[cell[0], cell[1], cell[2], 0:3] = reduced(cell)
        for which in some:
            source = tuple(
                pl.ds(size, 1) if bit else pl.ds(0, size)
                for bit, size in zip(corner_of(which), sizes)
            )
            copy = pltpu.make_async_remote_copy(
                src_ref=react.at[source],
                dst_ref=landed[which - 1],
                send_sem=back_send.at[which],
                recv_sem=back_recv.at[which],
                device_id=neighbour(which, 1),
                device_id_type=MESH,
            )
            copy.start()
            backs.append(copy)

    sums = across(sizes[1] * sizes[2], sheet, sums)
    give_back((1, 3, 5, 7))
    energy = lax.fori_loop(0, members, base_level, sums[0])
    sums = energy, sums[1]
    if less[0]:
        sums = across(bar + less[0] * less[1], border, sums)
    part[0:1] = jnp.sum(sums[0], 0, keepdims=True)
    part[1:2] = jnp.sum(sums[1], 0, keepdims=True)

    def send_plane():
        plane_copies = []
        for step in range(1, count_plane):
            copy = pltpu.make_async_remote_copy(
                src_ref=part if direct else middle,
                dst_ref=plane.at[at_plane],
                send_sem=plane_send.at[step],
                recv_sem=plane_recv.at[step],
                device_id=plane_target(step),
                device_id_type=MESH,
            )
            copy.start()
            plane_copies.append(copy)
        return plane_copies

    if direct:
        plane_copies = send_plane()
        plane[at_plane] = part[...]
    else:
        line_copies = []
        for step in range(1, count_x):
            copy = pltpu.make_async_remote_copy(
                src_ref=part,
                dst_ref=line.at[at_x],
                send_sem=line_send.at[step],
                recv_sem=line_recv.at[step],
                device_id=line_target(step),
                device_id_type=MESH,
            )
            copy.start()
            line_copies.append(copy)
        line[at_x] = part[...]
        for copy in line_copies:
            copy.wait()
        summed = line[0]
        for step in range(1, count_x):
            summed = summed + line[step]
        middle[...] = summed
        plane[at_plane] = summed
        plane_copies = send_plane()
    give_back((2, 4, 6))
    for cell in inner:
        react[cell[0], cell[1], cell[2], 0:3] = reduced(cell)
    for copy in backs:
        copy.wait()
    for x, y, z in inner:
        value = react[x, y, z]
        for which in range(1, 8):
            bits = corner_of(which)
            spot = (x, y, z)
            if all(not bit or at == 0 for bit, at in zip(bits, spot)):
                value = value + landed[which - 1][
                    tuple(0 if bit else at for bit, at in zip(bits, spot))
                ]
        for axis in range(3):
            at = ((axis * sizes[0] + x) * sizes[1] + y) * sizes[2] + z
            forces[pl.ds(at, 1)] = value[axis : axis + 1]
    for copy in plane_copies:
        copy.wait()
    summed = plane[0]
    for step in range(1, count_plane):
        summed = summed + plane[step]
    totals[0] = jnp.sum(summed[0:1]) * normaliser
    totals[1] = jnp.sum(summed[1:2]) * normaliser


def per_device(positions, type_ids, counts, type_charge, type_sigma, type_epsilon):
    types = type_charge.shape[0]
    sizes, width = type_ids.shape[:3], type_ids.shape[3]
    ext_sizes = tuple(size + 1 for size in sizes)
    cells = ext_sizes[0] * ext_sizes[1] * ext_sizes[2]
    members = sizes[0] * sizes[1] * sizes[2]
    vmem = pl.BlockSpec(memory_space=pltpu.VMEM)
    smem = pl.BlockSpec(memory_space=pltpu.SMEM)
    hbm = pl.BlockSpec(memory_space=pltpu.HBM)
    f32 = jnp.float32
    count_x, count_y, count_z = (lax.axis_size(axis) for axis in AXES)
    count_plane = count_y * count_z
    slots_x, slots_plane = count_x, count_plane
    if count_x * count_plane <= direct_limit:
        slots_x, slots_plane = 1, count_x * count_plane
    normaliser = 1.0 / (
        sizes[0] * count_x * sizes[1] * count_y * sizes[2] * count_z * width
    )
    landing = [
        pltpu.VMEM(
            tuple(1 if bit else size for bit, size in zip(corner_of(which), sizes)) + (4, width),
            f32,
        )
        for which in range(1, 8)
    ]
    counts = jnp.transpose(counts, (0, 2, 1))
    positions, type_ids, counts = (
        pltpu.with_memory_space_constraint(value, pltpu.HBM) for value in (positions, type_ids, counts)
    )
    type_charge, type_sigma, type_epsilon = (
        pltpu.with_memory_space_constraint(value, pltpu.HBM)
        for value in (type_charge, type_sigma, type_epsilon)
    )
    dma = pltpu.SemaphoreType.DMA
    forces, totals = pl.pallas_call(
        functools.partial(step_kernel, normaliser, types),
        name="step",
        out_shape=(
            jax.ShapeDtypeStruct((3 * members, width), f32),
            jax.ShapeDtypeStruct((2,), f32),
        ),
        in_specs=[smem, smem, smem, hbm, hbm, hbm],
        out_specs=(vmem, smem),
        scratch_shapes=[
            pltpu.VMEM(positions.shape, f32),
            pltpu.VMEM(type_ids.shape, jnp.int32),
            pltpu.VMEM(counts.shape, jnp.int32),
            pltpu.VMEM(sizes + (4, width), f32),
            pltpu.VMEM(ext_sizes + (4, width), f32),
            pltpu.VMEM((cells, width), f32),
            pltpu.VMEM((32, 4 * width), jnp.bfloat16),
            pltpu.VMEM((cells, width, 32), jnp.bfloat16),
            pltpu.VMEM((cells, 32, width), jnp.bfloat16),
            pltpu.VMEM((13, width // 8, 8, width), f32),
            pltpu.VMEM((13, width // 8, 8, width), f32),
            pltpu.VMEM((cells, 4, width // 8, 8, width), f32),
            pltpu.VMEM((cells, 3 + 5 * types, 8, width), f32),
            pltpu.VMEM((cells, types - 1, 8, width), f32),
            pltpu.VMEM((len(second_of), members, 3, width // 8, 8, width), f32),
            pltpu.VMEM((cells, 3, 8, width), f32),
            pltpu.VMEM(ext_sizes + (4, width), f32),
            pltpu.VMEM((2, width), f32),
            dma((3,)),
            dma((8,)),
            dma((8,)),
            dma((8,)),
            dma((8,)),
            pltpu.VMEM((slots_x, 2, width), f32),
            pltpu.VMEM((slots_plane, 2, width), f32),
            pltpu.VMEM((2, width), f32),
            dma((slots_x,)),
            dma((slots_x,)),
            dma((slots_plane,)),
            dma((slots_plane,)),
        ]
        + landing,
        compiler_params=pltpu.CompilerParams(
            collective_id=0, has_side_effects=True, vmem_limit_bytes=VMEM_LIMIT
        ),
    )(type_charge, type_sigma, type_epsilon, positions, type_ids, counts)
    return forces.reshape((3,) + sizes + (width,)), totals


def solution(mesh):
    in_specs = (
        P(None, "gx", "gy", "gz", None),
        P("gx", "gy", "gz", None),
        P("gx", "gy", "gz"),
        P(),
        P(),
        P(),
    )
    out_specs = (P(None, "gx", "gy", "gz", None), P())
    return jax.shard_map(
        per_device, mesh=mesh, in_specs=in_specs, out_specs=out_specs, check_vma=False
    )
```

```python
import functools

import jax
import jax.numpy as jnp
from jax import lax
from jax.experimental import pallas as pl
from jax.experimental.pallas import tpu as pltpu
from jax.sharding import PartitionSpec as P

MESH = pl.DeviceIdType.MESH
AXES = ("gx", "gy", "gz")
soft_core = 0.09
cut_sq = 1.0 + soft_core
cut_len = cut_sq**0.5
second_of = {0: (0, 1, 2, 3, 4, 5, 6, 7), 1: (2, 6), 2: (4, 5), 4: (1, 3)}
direct_limit = 64
far = 1024.0
VMEM_LIMIT = 40 * 1024 * 1024


def corner_of(which):
    return (which & 1, which >> 1 & 1, which >> 2 & 1)


def neighbour(which, step):
    target = {}
    for axis, bit in zip(AXES, corner_of(which)):
        if bit:
            count = lax.axis_size(axis)
            target[axis] = lax.rem(lax.axis_index(axis) + step + count, count)
    return target


def split(value):
    high = value.astype(jnp.bfloat16).astype(jnp.float32)
    rest = value - high
    middle = rest.astype(jnp.bfloat16).astype(jnp.float32)
    return high, middle, rest - middle


def type_tables(types, shape, charges, sigmas, epsilons):
    def full(value):
        return jnp.full(shape, value, jnp.float32)

    charge = [full(charges[kind]) for kind in range(types)]
    sigma = [full(sigmas[kind]) for kind in range(types)]
    root = [jnp.sqrt(full(epsilons[kind])) for kind in range(types)]
    tables = {}
    for a in range(types):
        for b in range(types):
            sigma_pair = 0.5 * (sigma[a] + sigma[b])
            depth_pair = 4.0 * root[a] * root[b]
            coulomb = charge[a] * charge[b]
            square = sigma_pair * sigma_pair
            sig_six = square * square * square
            six = 6.0 * depth_pair * sig_six
            twelve = 12.0 * depth_pair * sig_six * sig_six
            cut_six, cut_twelve, cut_coulomb = six * cut_sq**-3, twelve * cut_sq**-6, coulomb / cut_len
            shift = ((cut_six - cut_twelve) - cut_coulomb) / cut_len
            level = cut_len * shift - (cut_twelve / 12.0 - cut_six / 6.0 + cut_coulomb)
            tables[a, b] = (twelve, six, coulomb, shift, level)
    return tables


def step_kernel(
    normaliser, types, charge_all, sigma_all, epsilon_all, positions, type_ids, counts,
    forces, totals, charges, sigmas, epsilons, place_in, kind_in, count_in, own, ext, rows, pick, left, right, even, odd, first, table, number_of, force_i, force_j, react, part,
    in_sem, halo_send, halo_recv, back_send, back_recv,
    line, plane, middle, line_send, line_recv, plane_send, plane_recv, *landed,
):
    sizes = own.shape[:3]
    ext_sizes = ext.shape[:3]
    width = own.shape[-1]
    groups = width // 8
    per_cell = 3 + 5 * types
    members = sizes[0] * sizes[1] * sizes[2]
    count_x, count_y, count_z = (lax.axis_size(axis) for axis in AXES)
    at_x, at_y, at_z = (lax.axis_index(axis) for axis in AXES)
    count_plane = count_y * count_z
    at_plane = at_y * count_z + at_z
    direct = count_x * count_plane <= direct_limit
    loads = [
        pltpu.make_async_copy(source, target, in_sem.at[at])
        for at, (source, target) in enumerate(
            (
                (positions, place_in),
                (type_ids, kind_in),
                (counts, count_in),
                (charge_all, charges),
                (sigma_all, sigmas),
                (epsilon_all, epsilons),
            )
        )
    ]
    for load in loads:
        load.start()

    def around(at, count):
        return [at] + [at + step - count * (at + step >= count).astype(jnp.int32) for step in range(1, count)]

    spots = [around(at, count) for at, count in ((at_x, count_x), (at_y, count_y), (at_z, count_z))]
    if direct:
        count_plane, at_plane = count_x * count_plane, at_x * count_plane + at_plane
        count_x, at_x = 1, 0

    def line_target(step):
        return {"gx": spots[0][step]}

    def plane_target(step):
        target = {"gy": spots[1][step // count_z % count_y], "gz": spots[2][step % count_z]}
        if direct:
            target["gx"] = spots[0][step // (count_y * count_z)]
        return target

    barrier = pltpu.get_barrier_semaphore()
    greeted = count_x - 1 + count_plane - 1
    if not direct:
        greeted += 14
        for which in range(1, 8):
            for step in (1, -1):
                pl.semaphore_signal(barrier, inc=1, device_id=neighbour(which, step), device_id_type=MESH)
    for step in range(1, count_x):
        pl.semaphore_signal(barrier, inc=1, device_id=line_target(step), device_id_type=MESH)
    for step in range(1, count_plane):
        pl.semaphore_signal(barrier, inc=1, device_id=plane_target(step), device_id_type=MESH)

    cells = [
        (x, y, z)
        for x in range(ext_sizes[0])
        for y in range(ext_sizes[1])
        for z in range(ext_sizes[2])
    ]

    def outside(cell):
        return sum(at == size for at, size in zip(cell, sizes))

    def index_of(x, y, z):
        return (x * ext_sizes[1] + y) * ext_sizes[2] + z

    ordered = sorted(cells, key=outside)
    row_of = {cell: at for at, cell in enumerate(ordered)}
    inner = [cell for cell in ordered if outside(cell) == 0]
    outer = [cell for cell in ordered if outside(cell) > 0]

    force_j[...] = jnp.zeros(force_j.shape, jnp.float32)
    react[...] = jnp.zeros(react.shape, jnp.float32)
    slot = lax.broadcasted_iota(jnp.int32, (1, width), 1)

    for load in loads:
        load.wait()
    tables = type_tables(types, (8, width), charges, sigmas, epsilons)
    for x, y, z in inner:
        lines = [place_in[axis, x, y, pl.ds(z, 1)] for axis in range(3)]
        kind = kind_in[x, y, pl.ds(z, 1)].astype(jnp.float32)
        held = jnp.broadcast_to(count_in[x, pl.ds(z, 1), pl.ds(y, 1)], (1, width))
        lines.append(jnp.where(slot < held, kind, -1.0))
        tile = jnp.concatenate(lines, 0)
        own[x, y, z] = tile
        ext[x, y, z] = tile

    row = lax.broadcasted_iota(jnp.int32, (8, width), 0)
    low, top = row % 4, row < 4
    center = [0.5 * size for size in ext_sizes]
    wide_row = lax.broadcasted_iota(jnp.int32, (32, 4 * width), 0)
    wide_axis = lax.broadcasted_iota(jnp.int32, (32, 4 * width), 1) // width
    picked = (wide_row == wide_axis) | (wide_row == wide_axis + 8) | (wide_row == wide_axis + 20)
    picked = jnp.where(picked & (wide_axis < 3), 1.0, 0.0)
    picked = jnp.where((wide_axis == 3) & (wide_row == 27), 1.0, picked)
    pick[...] = picked.astype(jnp.bfloat16)

    def build(some):
        for x, y, z in some:
            cell = index_of(x, y, z)
            base = jnp.where(low == 0, x - center[0], jnp.where(low == 1, y - center[1], z - center[2]))
            lines = ext[x, y, z]
            rows[pl.ds(row_of[x, y, z], 1)] = lines[3:4]
            both = jnp.concatenate([lines, lines], 0)
            live = jnp.broadcast_to(lines[3:4], (8, width)) >= 0.0
            place = jnp.where(live & (low < 3), both + base, 0.0)
            for axis in range(3):
                table[cell, axis] = jnp.broadcast_to(place[axis : axis + 1], (8, width))
            norm = jnp.sum((place * place)[0:4], 0, keepdims=True)
            norm = jnp.where(live, jnp.broadcast_to(norm, (8, width)), far)
            high, mid, tiny = split(jnp.where(low == 3, norm, place))
            twice, twice_mid, twice_tiny = split(jnp.where(low == 3, norm + soft_core, -2.0 * place))
            high_one = jnp.where(row == 3, 1.0, high)
            twice_one = jnp.where(row == 3, 1.0, twice)
            right[cell] = jnp.concatenate(
                [
                    jnp.where(top, twice_one, jnp.where(row == 7, twice, twice_mid)),
                    jnp.where(top, twice_one, twice_mid),
                    jnp.where(top, twice_tiny, jnp.where(row == 7, 1.0, twice)),
                    jnp.zeros((8, width), jnp.float32),
                ],
                0,
            ).astype(jnp.bfloat16)
            if outside((x, y, z)) <= 1:
                turned = jnp.transpose(
                    jnp.concatenate(
                        [
                            jnp.where(row == 7, 1.0, high),
                            jnp.where(row == 7, 1.0, mid),
                            jnp.where(top, high_one, tiny),
                            both,
                        ],
                        0,
                    )
                )
                turned = turned.astype(jnp.bfloat16)
                left[cell] = turned
                spread = jnp.dot(turned, pick[...], preferred_element_type=jnp.float32)
                for axis in range(4):
                    first[cell, axis] = spread[:, axis * width : (axis + 1) * width].reshape(
                        (groups, 8, width)
                    )
            kind_row = jnp.broadcast_to(lines[3:4], (8, width))
            same = [kind_row == float(kind) for kind in range(types)]
            for kind in range(1, types):
                total = jnp.sum(same[kind].astype(jnp.float32), 1, keepdims=True) * 0.125
                number_of[cell, kind - 1] = jnp.broadcast_to(total, (8, width))
            for kind in range(types):
                for at in range(5):
                    picked = jnp.zeros((8, width), jnp.float32)
                    for second_kind in range(types):
                        picked = jnp.where(same[second_kind], tables[kind, second_kind][at], picked)
                    table[cell, 3 + 5 * kind + at] = picked

    build(inner)

    def interact(own_at, other, kinds, soft_sq, ordered=None):
        xi, yi, zi = own_at
        second = [table[other, at][None] for at in range(per_cell)]

        def chosen(at):
            value = second[3 + at]
            for kind in range(1, types):
                value = jnp.where(kinds[kind - 1], second[3 + 5 * kind + at], value)
            return value

        dx, dy, dz = second[0] - xi, second[1] - yi, second[2] - zi
        soft_sq = jnp.minimum(soft_sq, cut_sq)
        inverse = lax.rsqrt(soft_sq)
        inverse_2 = inverse * inverse
        inverse_6 = inverse_2 * inverse_2 * inverse_2
        twelve = chosen(0) * inverse_6 * inverse_6
        six = chosen(1) * inverse_6
        coulomb = chosen(2) * inverse
        shift = chosen(3) * (soft_sq * inverse)
        drive = (six - twelve) - (coulomb + shift)
        slope = drive * inverse_2
        forces = (slope * dx, slope * dy, slope * dz)
        for axis in range(3):
            force_j[other, axis] -= jnp.sum(forces[axis], 0)
        if ordered is None:
            terms = (twelve, six, coulomb, shift, slope)
            return forces, [jnp.sum(term, 0) for term in terms]
        value = twelve * (1.0 / 12.0) - six * (1.0 / 6.0) + coulomb - shift + chosen(4)
        pull = drive - soft_core * slope
        return [jnp.sum(jnp.where(ordered, term, 0.0), 0) for term in (value, pull)]

    def slots(depth):
        shape = (depth, 8, width)
        return (
            lax.broadcasted_iota(jnp.int32, shape, 0) * 8
            + lax.broadcasted_iota(jnp.int32, shape, 1)
            - lax.broadcasted_iota(jnp.int32, shape, 2)
        )

    def load_first(here, span):
        own_at = tuple(first[here, axis, span] for axis in range(3))
        kind_at = first[here, 3, span]
        return own_at, [kind_at == float(kind) for kind in range(1, types)]

    def alone(here, held, sums):
        slot_at = slots(4)
        for start in range(0, groups, 4):
            span = pl.ds(start, 4)
            own_at, kinds = load_first(here, span)
            values = interact(
                own_at, here, kinds, held[0, span], ordered=slot_at + start * 8 < 0
            )
            sums = tuple(a + b for a, b in zip(sums, values))
        return sums

    def apart(store, here):
        found = jnp.dot(left[here], right[here], preferred_element_type=jnp.float32)
        store[0] = found.reshape((groups, 8, width))

    def levels(energy, here, others):
        numbers = [number_of[here, kind - 1] for kind in range(1, types)]
        rest = jnp.full((8, width), float(groups))
        for number in numbers:
            rest = rest - number
        for other in others:
            for kind, number in enumerate([rest, *numbers]):
                energy = energy + number * table[other, 3 + 5 * kind + 4]
        return energy

    roles = {
        first_corner: tuple(which for which in seconds if which)
        for first_corner, seconds in second_of.items()
    }
    depth = 4
    trips = groups // depth
    offset_of = {}
    for first_corner, seconds in roles.items():
        offset_of[first_corner] = sum(len(roles[corner]) for corner in offset_of)

    def distances(store, cell_at, chunk, first_corner):
        wide = 8 * depth
        lefts = left[cell_at(first_corner), pl.ds(chunk * wide, wide)]
        seconds = roles[first_corner]
        for at in range(0, len(seconds), 2):
            some = [right[cell_at(which)] for which in seconds[at : at + 2]]
            found = jnp.dot(
                lefts,
                jnp.concatenate(some, 1) if len(some) > 1 else some[0],
                preferred_element_type=jnp.float32,
            )
            for n in range(len(some)):
                store[offset_of[first_corner] + at + n, pl.ds(chunk * depth, depth)] = found[:, n * width : (n + 1) * width].reshape(
                    (depth, 8, width)
                )

    def role(first_corner, member, cell_at, chunk, held, sums):
        here = cell_at(first_corner)
        part_at = tuple(second_of).index(first_corner)
        fine = 4 if first_corner == 0 else 4
        for start in range(0, depth, fine):
            span = pl.ds(chunk * depth + start, fine)
            own_at, kinds = load_first(here, span)
            total = None
            parts = None
            for n, which in enumerate(roles[first_corner]):
                forces, terms = interact(
                    own_at,
                    cell_at(which),
                    kinds,
                    held[offset_of[first_corner] + n, pl.ds(chunk * depth + start, fine)],
                )
                parts = terms if parts is None else [a + b for a, b in zip(parts, terms)]
                total = forces if total is None else [a + b for a, b in zip(total, forces)]
            twelve, six, coulomb, shift, slope = parts
            value = (twelve * (1.0 / 12.0) - six * (1.0 / 6.0)) + (coulomb - shift)
            pull = ((six - twelve) - (coulomb + shift)) - soft_core * slope
            for axis in range(3):
                force_i[part_at, member, axis, span] = total[axis]
            sums = sums[0] + value, sums[1] + pull
        return sums

    def corners(x0, y0, z0):
        def cell_at(which):
            shift = corner_of(which)
            return index_of(x0 + shift[0], y0 + shift[1], z0 + shift[2])

        return cell_at

    def one_pair(at, sums):
        cell = [
            index_of(
                member // (sizes[2] * sizes[1]),
                lax.rem(member // sizes[2], sizes[1]),
                lax.rem(member, sizes[2]),
            )
            for member in (2 * at, 2 * at + 1, jnp.minimum(2 * at + 2, members - 1))
        ]
        apart(odd, cell[1])
        sums = alone(cell[0], even, sums)
        apart(even, cell[2])
        return alone(cell[1], odd, sums)

    def across(homes, sums):
        stores = (even, odd)
        for first_corner in roles:
            for chunk in range(trips):
                distances(even, corners(*homes[0]), chunk, first_corner)
        for at, (x0, y0, z0) in enumerate(homes):
            member = (x0 * sizes[1] + y0) * sizes[2] + z0
            cell_at = corners(x0, y0, z0)
            held, store = stores[at % 2], stores[(at + 1) % 2]
            after = corners(*homes[at + 1]) if at + 1 < len(homes) else None

            def step(chunk, sums, some):
                for first_corner in some:
                    if after is not None:
                        distances(store, after, chunk, first_corner)
                for first_corner in some:
                    sums = role(first_corner, member, cell_at, chunk, held, sums)
                return sums

            for some in (tuple(roles),):
                sums = lax.fori_loop(0, trips, functools.partial(step, some=some), sums)
        return sums

    blank = jnp.zeros((8, width), jnp.float32)
    apart(even, index_of(0, 0, 0))
    sums = lax.fori_loop(0, members // 2, one_pair, (blank, blank))

    def base_level(member, energy):
        z0 = lax.rem(member, sizes[2])
        y0 = lax.rem(member // sizes[2], sizes[1])
        x0 = member // (sizes[2] * sizes[1])
        cell_at = corners(x0, y0, z0)
        for first_corner, seconds in roles.items():
            energy = levels(energy, cell_at(first_corner), [cell_at(which) for which in seconds])
        return energy


    pl.semaphore_wait(barrier, greeted)
    halos = []
    for which in range(1, 8):
        bits = corner_of(which)
        source = tuple(pl.ds(0, 1 if bit else size) for bit, size in zip(bits, sizes))
        target = tuple(
            pl.ds(size, 1) if bit else pl.ds(0, size) for bit, size in zip(bits, sizes)
        )
        copy = pltpu.make_async_remote_copy(
            src_ref=own.at[source],
            dst_ref=ext.at[target],
            send_sem=halo_send.at[which],
            recv_sem=halo_recv.at[which],
            device_id=neighbour(which, -1),
            device_id_type=MESH,
        )
        copy.start()
        halos.append(copy)

    less = tuple(size - 1 for size in sizes)

    homes = [
        (x, y, z) for x in range(sizes[0]) for y in range(sizes[1]) for z in range(sizes[2])
    ]
    inside = [home for home in homes if all(at < most for at, most in zip(home, less))]
    sheet = [home for home in homes if home[0] == less[0]]
    border = [home for home in homes if home not in inside and home not in sheet]
    if inside:
        sums = across(inside, sums)

    for copy in halos:
        copy.wait()
    build(outer)

    def reduced(cell):
        x, y, z = cell
        at_cell = index_of(x, y, z)
        held = rows[pl.ds(row_of[cell], 1)] >= 0.0
        lines = []
        for axis in range(3):
            line = force_j[at_cell, axis]
            partial = None
            for part_at, first_corner in enumerate(second_of):
                spot = [at - bit for at, bit in zip(cell, corner_of(first_corner))]
                if all(0 <= at < size for at, size in zip(spot, sizes)):
                    member = (spot[0] * sizes[1] + spot[1]) * sizes[2] + spot[2]
                    value = force_i[part_at, member, axis].reshape((width, width))
                    partial = value if partial is None else partial + value
            if partial is not None:
                turned = jnp.transpose(partial)
                line = line + jnp.sum(turned.reshape((groups, 8, width)), 0)
            line = jnp.sum(line, 0, keepdims=True)
            lines.append(jnp.where(held, line, 0.0))
        return jnp.concatenate(lines, 0)

    backs = []

    def give_back(some):
        for cell in outer:
            which = sum((at == size) << bit for bit, (at, size) in enumerate(zip(cell, sizes)))
            if which in some:
                react[cell[0], cell[1], cell[2], 0:3] = reduced(cell)
        for which in some:
            source = tuple(
                pl.ds(size, 1) if bit else pl.ds(0, size)
                for bit, size in zip(corner_of(which), sizes)
            )
            copy = pltpu.make_async_remote_copy(
                src_ref=react.at[source],
                dst_ref=landed[which - 1],
                send_sem=back_send.at[which],
                recv_sem=back_recv.at[which],
                device_id=neighbour(which, 1),
                device_id_type=MESH,
            )
            copy.start()
            backs.append(copy)

    sums = across(sheet, sums)
    give_back((1, 3, 5, 7))
    energy = lax.fori_loop(0, members, base_level, sums[0])
    sums = energy, sums[1]
    if border:
        sums = across(border, sums)
    part[0:1] = jnp.sum(sums[0], 0, keepdims=True)
    part[1:2] = jnp.sum(sums[1], 0, keepdims=True)

    def send_plane():
        plane_copies = []
        for step in range(1, count_plane):
            copy = pltpu.make_async_remote_copy(
                src_ref=part if direct else middle,
                dst_ref=plane.at[at_plane],
                send_sem=plane_send.at[step],
                recv_sem=plane_recv.at[step],
                device_id=plane_target(step),
                device_id_type=MESH,
            )
            copy.start()
            plane_copies.append(copy)
        return plane_copies

    if direct:
        plane_copies = send_plane()
        plane[at_plane] = part[...]
    else:
        line_copies = []
        for step in range(1, count_x):
            copy = pltpu.make_async_remote_copy(
                src_ref=part,
                dst_ref=line.at[at_x],
                send_sem=line_send.at[step],
                recv_sem=line_recv.at[step],
                device_id=line_target(step),
                device_id_type=MESH,
            )
            copy.start()
            line_copies.append(copy)
        line[at_x] = part[...]
        for copy in line_copies:
            copy.wait()
        summed = line[0]
        for step in range(1, count_x):
            summed = summed + line[step]
        middle[...] = summed
        plane[at_plane] = summed
        plane_copies = send_plane()
    give_back((2, 4, 6))
    for cell in inner:
        react[cell[0], cell[1], cell[2], 0:3] = reduced(cell)
    for copy in backs:
        copy.wait()
    for x, y, z in inner:
        value = react[x, y, z]
        for which in range(1, 8):
            bits = corner_of(which)
            spot = (x, y, z)
            if all(not bit or at == 0 for bit, at in zip(bits, spot)):
                value = value + landed[which - 1][
                    tuple(0 if bit else at for bit, at in zip(bits, spot))
                ]
        for axis in range(3):
            at = ((axis * sizes[0] + x) * sizes[1] + y) * sizes[2] + z
            forces[pl.ds(at, 1)] = value[axis : axis + 1]
    for copy in plane_copies:
        copy.wait()
    summed = plane[0]
    for step in range(1, count_plane):
        summed = summed + plane[step]
    totals[0] = jnp.sum(summed[0:1]) * normaliser
    totals[1] = jnp.sum(summed[1:2]) * normaliser


def per_device(positions, type_ids, counts, type_charge, type_sigma, type_epsilon):
    types = type_charge.shape[0]
    sizes, width = type_ids.shape[:3], type_ids.shape[3]
    ext_sizes = tuple(size + 1 for size in sizes)
    cells = ext_sizes[0] * ext_sizes[1] * ext_sizes[2]
    members = sizes[0] * sizes[1] * sizes[2]
    vmem = pl.BlockSpec(memory_space=pltpu.VMEM)
    smem = pl.BlockSpec(memory_space=pltpu.SMEM)
    hbm = pl.BlockSpec(memory_space=pltpu.HBM)
    f32 = jnp.float32
    count_x, count_y, count_z = (lax.axis_size(axis) for axis in AXES)
    count_plane = count_y * count_z
    slots_x, slots_plane = count_x, count_plane
    if count_x * count_plane <= direct_limit:
        slots_x, slots_plane = 1, count_x * count_plane
    normaliser = 1.0 / (
        sizes[0] * count_x * sizes[1] * count_y * sizes[2] * count_z * width
    )
    landing = [
        pltpu.VMEM(
            tuple(1 if bit else size for bit, size in zip(corner_of(which), sizes)) + (4, width),
            f32,
        )
        for which in range(1, 8)
    ]
    counts = jnp.transpose(counts, (0, 2, 1))
    positions, type_ids, counts = (
        pltpu.with_memory_space_constraint(value, pltpu.HBM) for value in (positions, type_ids, counts)
    )
    type_charge, type_sigma, type_epsilon = (
        pltpu.with_memory_space_constraint(value, pltpu.HBM)
        for value in (type_charge, type_sigma, type_epsilon)
    )
    dma = pltpu.SemaphoreType.DMA
    forces, totals = pl.pallas_call(
        functools.partial(step_kernel, normaliser, types),
        name="step",
        out_shape=(
            jax.ShapeDtypeStruct((3 * members, width), f32),
            jax.ShapeDtypeStruct((2,), f32),
        ),
        in_specs=[hbm] * 6,
        out_specs=(vmem, smem),
        scratch_shapes=[
            pltpu.SMEM((types,), f32),
            pltpu.SMEM((types,), f32),
            pltpu.SMEM((types,), f32),
            pltpu.VMEM(positions.shape, f32),
            pltpu.VMEM(type_ids.shape, jnp.int32),
            pltpu.VMEM(counts.shape, jnp.int32),
            pltpu.VMEM(sizes + (4, width), f32),
            pltpu.VMEM(ext_sizes + (4, width), f32),
            pltpu.VMEM((cells, width), f32),
            pltpu.VMEM((32, 4 * width), jnp.bfloat16),
            pltpu.VMEM((cells, width, 32), jnp.bfloat16),
            pltpu.VMEM((cells, 32, width), jnp.bfloat16),
            pltpu.VMEM((13, width // 8, 8, width), f32),
            pltpu.VMEM((13, width // 8, 8, width), f32),
            pltpu.VMEM((cells, 4, width // 8, 8, width), f32),
            pltpu.VMEM((cells, 3 + 5 * types, 8, width), f32),
            pltpu.VMEM((cells, types - 1, 8, width), f32),
            pltpu.VMEM((len(second_of), members, 3, width // 8, 8, width), f32),
            pltpu.VMEM((cells, 3, 8, width), f32),
            pltpu.VMEM(ext_sizes + (4, width), f32),
            pltpu.VMEM((2, width), f32),
            dma((6,)),
            dma((8,)),
            dma((8,)),
            dma((8,)),
            dma((8,)),
            pltpu.VMEM((slots_x, 2, width), f32),
            pltpu.VMEM((slots_plane, 2, width), f32),
            pltpu.VMEM((2, width), f32),
            dma((slots_x,)),
            dma((slots_x,)),
            dma((slots_plane,)),
            dma((slots_plane,)),
        ]
        + landing,
        compiler_params=pltpu.CompilerParams(
            collective_id=0, has_side_effects=True, vmem_limit_bytes=VMEM_LIMIT
        ),
    )(type_charge, type_sigma, type_epsilon, positions, type_ids, counts)
    return forces.reshape((3,) + sizes + (width,)), totals


def solution(mesh):
    in_specs = (
        P(None, "gx", "gy", "gz", None),
        P("gx", "gy", "gz", None),
        P("gx", "gy", "gz"),
        P(),
        P(),
        P(),
    )
    out_specs = (P(None, "gx", "gy", "gz", None), P())
    return jax.shard_map(
        per_device, mesh=mesh, in_specs=in_specs, out_specs=out_specs, check_vma=False
    )
```

```python
import functools

import jax
import jax.numpy as jnp
from jax import lax
from jax.experimental import pallas as pl
from jax.experimental.pallas import tpu as pltpu
from jax.sharding import PartitionSpec as P

MESH = pl.DeviceIdType.MESH
AXES = ("gx", "gy", "gz")
soft_core = 0.09
cut_sq = 1.0 + soft_core
cut_len = cut_sq**0.5
second_of = {0: (0, 1, 2, 3, 4, 5, 6, 7), 1: (2, 6), 2: (4, 5), 4: (1, 3)}
direct_limit = 64
far = 1024.0
VMEM_LIMIT = 40 * 1024 * 1024


def corner_of(which):
    return (which & 1, which >> 1 & 1, which >> 2 & 1)


def neighbour(which, step):
    target = {}
    for axis, bit in zip(AXES, corner_of(which)):
        if bit:
            count = lax.axis_size(axis)
            target[axis] = lax.rem(lax.axis_index(axis) + step + count, count)
    return target


def split(value):
    high = value.astype(jnp.bfloat16).astype(jnp.float32)
    rest = value - high
    middle = rest.astype(jnp.bfloat16).astype(jnp.float32)
    return high, middle, rest - middle


def type_tables(types, shape, charges, sigmas, epsilons):
    def full(value):
        return jnp.full(shape, value, jnp.float32)

    charge = [full(charges[kind]) for kind in range(types)]
    sigma = [full(sigmas[kind]) for kind in range(types)]
    root = [jnp.sqrt(full(epsilons[kind])) for kind in range(types)]
    tables = {}
    for a in range(types):
        for b in range(types):
            sigma_pair = 0.5 * (sigma[a] + sigma[b])
            depth_pair = 4.0 * root[a] * root[b]
            coulomb = charge[a] * charge[b]
            square = sigma_pair * sigma_pair
            sig_six = square * square * square
            six = 6.0 * depth_pair * sig_six
            twelve = 12.0 * depth_pair * sig_six * sig_six
            cut_six, cut_twelve, cut_coulomb = six * cut_sq**-3, twelve * cut_sq**-6, coulomb / cut_len
            shift = ((cut_six - cut_twelve) - cut_coulomb) / cut_len
            level = cut_len * shift - (cut_twelve / 12.0 - cut_six / 6.0 + cut_coulomb)
            tables[a, b] = (twelve, six, coulomb, shift, level)
    return tables


def step_kernel(
    normaliser, types, charge_all, sigma_all, epsilon_all, positions, type_ids, counts,
    forces, totals, charges, sigmas, epsilons, place_in, kind_in, count_in, own, ext, rows, pick, left, right, even, odd, first, table, number_of, force_i, force_j, react, part,
    in_sem, halo_send, halo_recv, back_send, back_recv,
    line, plane, middle, line_send, line_recv, plane_send, plane_recv, *landed,
):
    sizes = own.shape[:3]
    ext_sizes = ext.shape[:3]
    width = own.shape[-1]
    groups = width // 8
    per_cell = 3 + 5 * types
    members = sizes[0] * sizes[1] * sizes[2]
    count_x, count_y, count_z = (lax.axis_size(axis) for axis in AXES)
    at_x, at_y, at_z = (lax.axis_index(axis) for axis in AXES)
    count_plane = count_y * count_z
    at_plane = at_y * count_z + at_z
    direct = count_x * count_plane <= direct_limit
    loads = [
        pltpu.make_async_copy(source, target, in_sem.at[at])
        for at, (source, target) in enumerate(
            (
                (positions, place_in),
                (type_ids, kind_in),
                (counts, count_in),
                (charge_all, charges),
                (sigma_all, sigmas),
                (epsilon_all, epsilons),
            )
        )
    ]
    for load in loads:
        load.start()

    def around(at, count):
        return [at] + [at + step - count * (at + step >= count).astype(jnp.int32) for step in range(1, count)]

    spots = [around(at, count) for at, count in ((at_x, count_x), (at_y, count_y), (at_z, count_z))]
    if direct:
        count_plane, at_plane = count_x * count_plane, at_x * count_plane + at_plane
        count_x, at_x = 1, 0

    def line_target(step):
        return {"gx": spots[0][step]}

    def plane_target(step):
        target = {"gy": spots[1][step // count_z % count_y], "gz": spots[2][step % count_z]}
        if direct:
            target["gx"] = spots[0][step // (count_y * count_z)]
        return target

    barrier = pltpu.get_barrier_semaphore()
    greeted = count_x - 1 + count_plane - 1
    if not direct:
        greeted += 14
        for which in range(1, 8):
            for step in (1, -1):
                pl.semaphore_signal(barrier, inc=1, device_id=neighbour(which, step), device_id_type=MESH)
    for step in range(1, count_x):
        pl.semaphore_signal(barrier, inc=1, device_id=line_target(step), device_id_type=MESH)
    for step in range(1, count_plane):
        pl.semaphore_signal(barrier, inc=1, device_id=plane_target(step), device_id_type=MESH)

    cells = [
        (x, y, z)
        for x in range(ext_sizes[0])
        for y in range(ext_sizes[1])
        for z in range(ext_sizes[2])
    ]

    def outside(cell):
        return sum(at == size for at, size in zip(cell, sizes))

    def index_of(x, y, z):
        return (x * ext_sizes[1] + y) * ext_sizes[2] + z

    ordered = sorted(cells, key=outside)
    row_of = {cell: at for at, cell in enumerate(ordered)}
    inner = [cell for cell in ordered if outside(cell) == 0]
    outer = [cell for cell in ordered if outside(cell) > 0]

    force_j[...] = jnp.zeros(force_j.shape, jnp.float32)
    react[...] = jnp.zeros(react.shape, jnp.float32)
    slot = lax.broadcasted_iota(jnp.int32, (1, width), 1)

    for load in loads:
        load.wait()
    tables = type_tables(types, (8, width), charges, sigmas, epsilons)
    for x, y, z in inner:
        lines = [place_in[axis, x, y, pl.ds(z, 1)] for axis in range(3)]
        kind = kind_in[x, y, pl.ds(z, 1)].astype(jnp.float32)
        held = jnp.broadcast_to(count_in[x, pl.ds(z, 1), pl.ds(y, 1)], (1, width))
        lines.append(jnp.where(slot < held, kind, -1.0))
        tile = jnp.concatenate(lines, 0)
        own[x, y, z] = tile
        ext[x, y, z] = tile

    row = lax.broadcasted_iota(jnp.int32, (8, width), 0)
    low, top = row % 4, row < 4
    center = [0.5 * size for size in ext_sizes]
    wide_row = lax.broadcasted_iota(jnp.int32, (32, 4 * width), 0)
    wide_axis = lax.broadcasted_iota(jnp.int32, (32, 4 * width), 1) // width
    picked = (wide_row == wide_axis) | (wide_row == wide_axis + 8) | (wide_row == wide_axis + 20)
    picked = jnp.where(picked & (wide_axis < 3), 1.0, 0.0)
    picked = jnp.where((wide_axis == 3) & (wide_row == 27), 1.0, picked)
    pick[...] = picked.astype(jnp.bfloat16)

    def build(some):
        for x, y, z in some:
            cell = index_of(x, y, z)
            base = jnp.where(low == 0, x - center[0], jnp.where(low == 1, y - center[1], z - center[2]))
            lines = ext[x, y, z]
            rows[pl.ds(row_of[x, y, z], 1)] = lines[3:4]
            both = jnp.concatenate([lines, lines], 0)
            live = jnp.broadcast_to(lines[3:4], (8, width)) >= 0.0
            place = jnp.where(live & (low < 3), both + base, 0.0)
            for axis in range(3):
                table[cell, axis] = jnp.broadcast_to(place[axis : axis + 1], (8, width))
            norm = jnp.sum((place * place)[0:4], 0, keepdims=True)
            norm = jnp.where(live, jnp.broadcast_to(norm, (8, width)), far)
            high, mid, tiny = split(jnp.where(low == 3, norm, place))
            twice, twice_mid, twice_tiny = split(jnp.where(low == 3, norm + soft_core, -2.0 * place))
            high_one = jnp.where(row == 3, 1.0, high)
            twice_one = jnp.where(row == 3, 1.0, twice)
            right[cell] = jnp.concatenate(
                [
                    jnp.where(top, twice_one, jnp.where(row == 7, twice, twice_mid)),
                    jnp.where(top, twice_one, twice_mid),
                    jnp.where(top, twice_tiny, jnp.where(row == 7, 1.0, twice)),
                    jnp.zeros((8, width), jnp.float32),
                ],
                0,
            ).astype(jnp.bfloat16)
            if outside((x, y, z)) <= 1:
                turned = jnp.transpose(
                    jnp.concatenate(
                        [
                            jnp.where(row == 7, 1.0, high),
                            jnp.where(row == 7, 1.0, mid),
                            jnp.where(top, high_one, tiny),
                            both,
                        ],
                        0,
                    )
                )
                turned = turned.astype(jnp.bfloat16)
                left[cell] = turned
                spread = jnp.dot(turned, pick[...], preferred_element_type=jnp.float32)
                for axis in range(4):
                    first[cell, axis] = spread[:, axis * width : (axis + 1) * width].reshape(
                        (groups, 8, width)
                    )
            kind_row = jnp.broadcast_to(lines[3:4], (8, width))
            same = [kind_row == float(kind) for kind in range(types)]
            for kind in range(1, types):
                total = jnp.sum(same[kind].astype(jnp.float32), 1, keepdims=True) * 0.125
                number_of[cell, kind - 1] = jnp.broadcast_to(total, (8, width))
            for kind in range(types):
                for at in range(5):
                    picked = jnp.zeros((8, width), jnp.float32)
                    for second_kind in range(types):
                        picked = jnp.where(same[second_kind], tables[kind, second_kind][at], picked)
                    table[cell, 3 + 5 * kind + at] = picked

    build(inner)

    def interact(own_at, other, kinds, soft_sq, ordered=None):
        xi, yi, zi = own_at
        second = [table[other, at][None] for at in range(per_cell)]

        def chosen(at):
            value = second[3 + at]
            for kind in range(1, types):
                value = jnp.where(kinds[kind - 1], second[3 + 5 * kind + at], value)
            return value

        dx, dy, dz = second[0] - xi, second[1] - yi, second[2] - zi
        soft_sq = jnp.minimum(soft_sq, cut_sq)
        inverse = lax.rsqrt(soft_sq)
        inverse_2 = inverse * inverse
        inverse_6 = inverse_2 * inverse_2 * inverse_2
        twelve = chosen(0) * inverse_6 * inverse_6
        six = chosen(1) * inverse_6
        coulomb = chosen(2) * inverse
        shift = chosen(3) * (soft_sq * inverse)
        drive = (six - twelve) - (coulomb + shift)
        slope = drive * inverse_2
        forces = (slope * dx, slope * dy, slope * dz)
        for axis in range(3):
            force_j[other, axis] -= jnp.sum(forces[axis], 0)
        if ordered is None:
            terms = (twelve, six, coulomb, shift, slope)
            return forces, [jnp.sum(term, 0) for term in terms]
        value = twelve * (1.0 / 12.0) - six * (1.0 / 6.0) + coulomb - shift + chosen(4)
        pull = drive - soft_core * slope
        return [jnp.sum(jnp.where(ordered, term, 0.0), 0) for term in (value, pull)]

    def slots(depth):
        shape = (depth, 8, width)
        return (
            lax.broadcasted_iota(jnp.int32, shape, 0) * 8
            + lax.broadcasted_iota(jnp.int32, shape, 1)
            - lax.broadcasted_iota(jnp.int32, shape, 2)
        )

    def load_first(here, span):
        own_at = tuple(first[here, axis, span] for axis in range(3))
        kind_at = first[here, 3, span]
        return own_at, [kind_at == float(kind) for kind in range(1, types)]

    def alone(here, held, sums):
        slot_at = slots(4)
        for start in range(0, groups, 4):
            span = pl.ds(start, 4)
            own_at, kinds = load_first(here, span)
            values = interact(
                own_at, here, kinds, held[0, span], ordered=slot_at + start * 8 < 0
            )
            sums = tuple(a + b for a, b in zip(sums, values))
        return sums

    def apart(store, here):
        found = jnp.dot(left[here], right[here], preferred_element_type=jnp.float32)
        store[0] = found.reshape((groups, 8, width))

    def levels(energy, here, others):
        numbers = [number_of[here, kind - 1] for kind in range(1, types)]
        rest = jnp.full((8, width), float(groups))
        for number in numbers:
            rest = rest - number
        for other in others:
            for kind, number in enumerate([rest, *numbers]):
                energy = energy + number * table[other, 3 + 5 * kind + 4]
        return energy

    roles = {
        first_corner: tuple(which for which in seconds if which)
        for first_corner, seconds in second_of.items()
    }
    depth = 4
    trips = groups // depth
    offset_of = {}
    for first_corner, seconds in roles.items():
        offset_of[first_corner] = sum(len(roles[corner]) for corner in offset_of)

    def distances(store, cell_at, chunk, first_corner):
        wide = 8 * depth
        lefts = left[cell_at(first_corner), pl.ds(chunk * wide, wide)]
        seconds = roles[first_corner]
        for at in range(0, len(seconds), 2):
            some = [right[cell_at(which)] for which in seconds[at : at + 2]]
            found = jnp.dot(
                lefts,
                jnp.concatenate(some, 1) if len(some) > 1 else some[0],
                preferred_element_type=jnp.float32,
            )
            for n in range(len(some)):
                store[offset_of[first_corner] + at + n, pl.ds(chunk * depth, depth)] = found[:, n * width : (n + 1) * width].reshape(
                    (depth, 8, width)
                )

    def role(first_corner, member, cell_at, chunk, held, sums):
        here = cell_at(first_corner)
        part_at = tuple(second_of).index(first_corner)
        fine = 4 if first_corner == 0 else 4
        for start in range(0, depth, fine):
            span = pl.ds(chunk * depth + start, fine)
            own_at, kinds = load_first(here, span)
            total = None
            parts = None
            for n, which in enumerate(roles[first_corner]):
                forces, terms = interact(
                    own_at,
                    cell_at(which),
                    kinds,
                    held[offset_of[first_corner] + n, pl.ds(chunk * depth + start, fine)],
                )
                parts = terms if parts is None else [a + b for a, b in zip(parts, terms)]
                total = forces if total is None else [a + b for a, b in zip(total, forces)]
            twelve, six, coulomb, shift, slope = parts
            value = (twelve * (1.0 / 12.0) - six * (1.0 / 6.0)) + (coulomb - shift)
            pull = ((six - twelve) - (coulomb + shift)) - soft_core * slope
            for axis in range(3):
                force_i[part_at, member, axis, span] = total[axis]
            sums = sums[0] + value, sums[1] + pull
        return sums

    def corners(x0, y0, z0):
        def cell_at(which):
            shift = corner_of(which)
            return index_of(x0 + shift[0], y0 + shift[1], z0 + shift[2])

        return cell_at

    def one_pair(at, sums):
        cell = [
            index_of(
                member // (sizes[2] * sizes[1]),
                lax.rem(member // sizes[2], sizes[1]),
                lax.rem(member, sizes[2]),
            )
            for member in (2 * at, 2 * at + 1, jnp.minimum(2 * at + 2, members - 1))
        ]
        apart(odd, cell[1])
        sums = alone(cell[0], even, sums)
        apart(even, cell[2])
        return alone(cell[1], odd, sums)

    def across(homes, sums, pause=None, then=None):
        stores = (even, odd)
        for first_corner in roles:
            for chunk in range(trips):
                distances(even, corners(*homes[0]), chunk, first_corner)
        for at, (x0, y0, z0) in enumerate(homes):
            if at == pause:
                then()
            member = (x0 * sizes[1] + y0) * sizes[2] + z0
            cell_at = corners(x0, y0, z0)
            held, store = stores[at % 2], stores[(at + 1) % 2]
            after = corners(*homes[at + 1]) if at + 1 < len(homes) else None

            def step(chunk, sums, some):
                for first_corner in some:
                    if after is not None:
                        distances(store, after, chunk, first_corner)
                for first_corner in some:
                    sums = role(first_corner, member, cell_at, chunk, held, sums)
                return sums

            for some in (tuple(roles),):
                sums = lax.fori_loop(0, trips, functools.partial(step, some=some), sums)
        return sums

    blank = jnp.zeros((8, width), jnp.float32)
    apart(even, index_of(0, 0, 0))
    sums = lax.fori_loop(0, members // 2, one_pair, (blank, blank))

    def base_level(member, energy):
        z0 = lax.rem(member, sizes[2])
        y0 = lax.rem(member // sizes[2], sizes[1])
        x0 = member // (sizes[2] * sizes[1])
        cell_at = corners(x0, y0, z0)
        for first_corner, seconds in roles.items():
            energy = levels(energy, cell_at(first_corner), [cell_at(which) for which in seconds])
        return energy


    pl.semaphore_wait(barrier, greeted)
    halos = []
    for which in range(1, 8):
        bits = corner_of(which)
        source = tuple(pl.ds(0, 1 if bit else size) for bit, size in zip(bits, sizes))
        target = tuple(
            pl.ds(size, 1) if bit else pl.ds(0, size) for bit, size in zip(bits, sizes)
        )
        copy = pltpu.make_async_remote_copy(
            src_ref=own.at[source],
            dst_ref=ext.at[target],
            send_sem=halo_send.at[which],
            recv_sem=halo_recv.at[which],
            device_id=neighbour(which, -1),
            device_id_type=MESH,
        )
        copy.start()
        halos.append(copy)

    less = tuple(size - 1 for size in sizes)

    homes = [
        (x, y, z) for x in range(sizes[0]) for y in range(sizes[1]) for z in range(sizes[2])
    ]
    inside = [home for home in homes if all(at < most for at, most in zip(home, less))]
    sheet = [home for home in homes if home[0] == less[0]]
    border = [home for home in homes if home not in inside and home not in sheet]
    if inside:
        sums = across(inside, sums)

    for copy in halos:
        copy.wait()
    build(outer)

    def reduced(cell):
        x, y, z = cell
        at_cell = index_of(x, y, z)
        held = rows[pl.ds(row_of[cell], 1)] >= 0.0
        lines = []
        for axis in range(3):
            line = force_j[at_cell, axis]
            partial = None
            for part_at, first_corner in enumerate(second_of):
                spot = [at - bit for at, bit in zip(cell, corner_of(first_corner))]
                if all(0 <= at < size for at, size in zip(spot, sizes)):
                    member = (spot[0] * sizes[1] + spot[1]) * sizes[2] + spot[2]
                    value = force_i[part_at, member, axis].reshape((width, width))
                    partial = value if partial is None else partial + value
            if partial is not None:
                turned = jnp.transpose(partial)
                line = line + jnp.sum(turned.reshape((groups, 8, width)), 0)
            line = jnp.sum(line, 0, keepdims=True)
            lines.append(jnp.where(held, line, 0.0))
        return jnp.concatenate(lines, 0)

    backs = []

    def give_back(some):
        for cell in outer:
            which = sum((at == size) << bit for bit, (at, size) in enumerate(zip(cell, sizes)))
            if which in some:
                react[cell[0], cell[1], cell[2], 0:3] = reduced(cell)
        for which in some:
            source = tuple(
                pl.ds(size, 1) if bit else pl.ds(0, size)
                for bit, size in zip(corner_of(which), sizes)
            )
            copy = pltpu.make_async_remote_copy(
                src_ref=react.at[source],
                dst_ref=landed[which - 1],
                send_sem=back_send.at[which],
                recv_sem=back_recv.at[which],
                device_id=neighbour(which, 1),
                device_id_type=MESH,
            )
            copy.start()
            backs.append(copy)

    energy = lax.fori_loop(0, members, base_level, sums[0])
    far_side = functools.partial(give_back, (1, 3, 5, 7))
    sums = across(sheet + border, (energy, sums[1]), len(sheet), far_side)
    if not border:
        far_side()
    part[0:1] = jnp.sum(sums[0], 0, keepdims=True)
    part[1:2] = jnp.sum(sums[1], 0, keepdims=True)

    def send_plane():
        plane_copies = []
        for step in range(1, count_plane):
            copy = pltpu.make_async_remote_copy(
                src_ref=part if direct else middle,
                dst_ref=plane.at[at_plane],
                send_sem=plane_send.at[step],
                recv_sem=plane_recv.at[step],
                device_id=plane_target(step),
                device_id_type=MESH,
            )
            copy.start()
            plane_copies.append(copy)
        return plane_copies

    if direct:
        plane_copies = send_plane()
        plane[at_plane] = part[...]
    else:
        line_copies = []
        for step in range(1, count_x):
            copy = pltpu.make_async_remote_copy(
                src_ref=part,
                dst_ref=line.at[at_x],
                send_sem=line_send.at[step],
                recv_sem=line_recv.at[step],
                device_id=line_target(step),
                device_id_type=MESH,
            )
            copy.start()
            line_copies.append(copy)
        line[at_x] = part[...]
        for copy in line_copies:
            copy.wait()
        summed = line[0]
        for step in range(1, count_x):
            summed = summed + line[step]
        middle[...] = summed
        plane[at_plane] = summed
        plane_copies = send_plane()
    give_back((2, 4, 6))
    for cell in inner:
        react[cell[0], cell[1], cell[2], 0:3] = reduced(cell)
    for copy in backs:
        copy.wait()
    for x, y, z in inner:
        value = react[x, y, z]
        for which in range(1, 8):
            bits = corner_of(which)
            spot = (x, y, z)
            if all(not bit or at == 0 for bit, at in zip(bits, spot)):
                value = value + landed[which - 1][
                    tuple(0 if bit else at for bit, at in zip(bits, spot))
                ]
        for axis in range(3):
            at = ((axis * sizes[0] + x) * sizes[1] + y) * sizes[2] + z
            forces[pl.ds(at, 1)] = value[axis : axis + 1]
    for copy in plane_copies:
        copy.wait()
    summed = jnp.sum(plane[...], 0)
    whole = jnp.sum(summed, 1, keepdims=True) * normaliser
    totals[...] = jnp.broadcast_to(whole, totals.shape)


def per_device(positions, type_ids, counts, type_charge, type_sigma, type_epsilon):
    types = type_charge.shape[0]
    sizes, width = type_ids.shape[:3], type_ids.shape[3]
    ext_sizes = tuple(size + 1 for size in sizes)
    cells = ext_sizes[0] * ext_sizes[1] * ext_sizes[2]
    members = sizes[0] * sizes[1] * sizes[2]
    vmem = pl.BlockSpec(memory_space=pltpu.VMEM)
    hbm = pl.BlockSpec(memory_space=pltpu.HBM)
    f32 = jnp.float32
    count_x, count_y, count_z = (lax.axis_size(axis) for axis in AXES)
    count_plane = count_y * count_z
    slots_x, slots_plane = count_x, count_plane
    if count_x * count_plane <= direct_limit:
        slots_x, slots_plane = 1, count_x * count_plane
    normaliser = 1.0 / (
        sizes[0] * count_x * sizes[1] * count_y * sizes[2] * count_z * width
    )
    landing = [
        pltpu.VMEM(
            tuple(1 if bit else size for bit, size in zip(corner_of(which), sizes)) + (4, width),
            f32,
        )
        for which in range(1, 8)
    ]
    counts = jnp.transpose(counts, (0, 2, 1))
    positions, type_ids, counts = (
        pltpu.with_memory_space_constraint(value, pltpu.HBM) for value in (positions, type_ids, counts)
    )
    type_charge, type_sigma, type_epsilon = (
        pltpu.with_memory_space_constraint(value, pltpu.HBM)
        for value in (type_charge, type_sigma, type_epsilon)
    )
    dma = pltpu.SemaphoreType.DMA
    forces, totals = pl.pallas_call(
        functools.partial(step_kernel, normaliser, types),
        name="step",
        out_shape=(
            jax.ShapeDtypeStruct((3 * members, width), f32),
            jax.ShapeDtypeStruct((2, width), f32),
        ),
        in_specs=[hbm] * 6,
        out_specs=(vmem, vmem),
        scratch_shapes=[
            pltpu.SMEM((types,), f32),
            pltpu.SMEM((types,), f32),
            pltpu.SMEM((types,), f32),
            pltpu.VMEM(positions.shape, f32),
            pltpu.VMEM(type_ids.shape, jnp.int32),
            pltpu.VMEM(counts.shape, jnp.int32),
            pltpu.VMEM(sizes + (4, width), f32),
            pltpu.VMEM(ext_sizes + (4, width), f32),
            pltpu.VMEM((cells, width), f32),
            pltpu.VMEM((32, 4 * width), jnp.bfloat16),
            pltpu.VMEM((cells, width, 32), jnp.bfloat16),
            pltpu.VMEM((cells, 32, width), jnp.bfloat16),
            pltpu.VMEM((13, width // 8, 8, width), f32),
            pltpu.VMEM((13, width // 8, 8, width), f32),
            pltpu.VMEM((cells, 4, width // 8, 8, width), f32),
            pltpu.VMEM((cells, 3 + 5 * types, 8, width), f32),
            pltpu.VMEM((cells, types - 1, 8, width), f32),
            pltpu.VMEM((len(second_of), members, 3, width // 8, 8, width), f32),
            pltpu.VMEM((cells, 3, 8, width), f32),
            pltpu.VMEM(ext_sizes + (4, width), f32),
            pltpu.VMEM((2, width), f32),
            dma((6,)),
            dma((8,)),
            dma((8,)),
            dma((8,)),
            dma((8,)),
            pltpu.VMEM((slots_x, 2, width), f32),
            pltpu.VMEM((slots_plane, 2, width), f32),
            pltpu.VMEM((2, width), f32),
            dma((slots_x,)),
            dma((slots_x,)),
            dma((slots_plane,)),
            dma((slots_plane,)),
        ]
        + landing,
        compiler_params=pltpu.CompilerParams(
            collective_id=0, has_side_effects=True, vmem_limit_bytes=VMEM_LIMIT
        ),
    )(type_charge, type_sigma, type_epsilon, positions, type_ids, counts)
    return forces.reshape((3,) + sizes + (width,)), totals[:, 0]


def solution(mesh):
    in_specs = (
        P(None, "gx", "gy", "gz", None),
        P("gx", "gy", "gz", None),
        P("gx", "gy", "gz"),
        P(),
        P(),
        P(),
    )
    out_specs = (P(None, "gx", "gy", "gz", None), P())
    return jax.shard_map(
        per_device, mesh=mesh, in_specs=in_specs, out_specs=out_specs, check_vma=False
    )
```
